8 devices in a mesh: data: 2 (over z, y), seq: 4 (over x, core).
Axes of the slice: x: 2, y: 2, z: 1, core: 2. Of those that a mesh axis runs over, the one named last changes fastest.
Arguments:
- x_tokens: bfloat16 [128, 512, 768], P('data', 'seq'), parts along dimension 0
- lengths: int32 [128], P('data'), parts along dimension 0
- phi_slots: bfloat16 [768, 128], replicated
- scale_g: float32 [], replicated
- w_in: bfloat16 [128, 768, 3072], P('seq')
- w_out: bfloat16 [128, 3072, 768], P('seq')
- ws_in: bfloat16 [768, 3072], replicated
- ws_out: bfloat16 [3072, 768], replicated
Outputs:
- output: bfloat16 [128, 512, 768], P('data', 'seq'), parts along dimension 0
There are 2 independent parts. The reference program is written for one: setup_inputs(seed, part) draws one part's arguments, and reference() takes and returns one part's arrays. A program takes and returns all parts, laid end to end along the dimension named above; an argument that names none is the same for every part.
All inputs are finite; a program needn't handle non-finite values.
Results may differ from the reference program's by a relative error of at most 0.0133234.
Values are sent between devices in bfloat16 or wider.
A program may use at most 1.5 GiB of HBM per device.

```python
import jax
import jax.numpy as jnp
from jax import lax

SEQ_BATCH = 64
SEQ_LEN = 512
MODEL_DIM = 768
EXPERT_FF = 3072
NUM_EXPERTS = 128
EXPERT_SLOTS = 1
SHARED_FF = 3072
SLOT_TOTAL = NUM_EXPERTS * EXPERT_SLOTS
NORM_EPS = 1e-6
NEG_BIG = -1e30


def setup_inputs(seed: int = 0, part: int = 0) -> dict:
    root_key = jax.random.key(seed)
    shared_keys = jax.random.split(root_key, 6)
    part_keys = jax.random.split(jax.random.fold_in(root_key, part), 5)
    phi_wide = jax.random.normal(shared_keys[0], (MODEL_DIM, SLOT_TOTAL), jnp.float32)
    phi_unit = phi_wide / jnp.sqrt(jnp.sum(phi_wide * phi_wide, axis=0, keepdims=True))
    slot_pick = jax.random.randint(part_keys[0], (SEQ_BATCH, SEQ_LEN), 0, SLOT_TOTAL)
    align_amp = jax.random.uniform(part_keys[1], (SEQ_BATCH, SEQ_LEN, 1), jnp.float32, 0.0, 2.0)
    noise_part = jax.random.normal(part_keys[2], (SEQ_BATCH, SEQ_LEN, MODEL_DIM), jnp.float32)
    x_wide = noise_part + jnp.take(phi_unit.T, slot_pick, axis=0) * (align_amp * MODEL_DIM ** 0.5)
    base_len = jax.random.randint(part_keys[3], (SEQ_BATCH,), 1, SEQ_LEN + 1)
    full_idx = jax.random.randint(part_keys[4], (), 0, SEQ_BATCH)
    lengths = jnp.where(jnp.arange(SEQ_BATCH) == full_idx, SEQ_LEN, base_len).astype(jnp.int32)
    scale_g = jax.random.uniform(shared_keys[1], (), jnp.float32, 4.0, 8.0)
    w_in = jax.random.normal(shared_keys[2], (NUM_EXPERTS, MODEL_DIM, EXPERT_FF), jnp.float32) * MODEL_DIM ** -0.5
    w_out = jax.random.normal(shared_keys[3], (NUM_EXPERTS, EXPERT_FF, MODEL_DIM), jnp.float32) * (2.0 * EXPERT_FF ** -0.5)
    ws_in = jax.random.normal(shared_keys[4], (MODEL_DIM, SHARED_FF), jnp.float32)
    ws_out = jax.random.normal(shared_keys[5], (SHARED_FF, MODEL_DIM), jnp.float32) * (0.25 * SHARED_FF ** -0.5)
    return {'x_tokens': x_wide.astype(jnp.bfloat16), 'lengths': lengths, 'phi_slots': phi_wide.astype(jnp.bfloat16), 'scale_g': scale_g, 'w_in': w_in.astype(jnp.bfloat16), 'w_out': w_out.astype(jnp.bfloat16), 'ws_in': ws_in.astype(jnp.bfloat16), 'ws_out': ws_out.astype(jnp.bfloat16)}


def unit_rows(values, axis_id):
    wide_vals = values.astype(jnp.float32)
    return wide_vals / jnp.sqrt(jnp.sum(wide_vals * wide_vals, axis=axis_id, keepdims=True) + NORM_EPS)


def reference(x_tokens, lengths, phi_slots, scale_g, w_in, w_out, ws_in, ws_out):
    phi_norm = (scale_g * unit_rows(phi_slots, 0)).astype(jnp.bfloat16)
    positions = jnp.arange(SEQ_LEN)

    def seq_logits(x_seq):
        x_unit = unit_rows(x_seq, 1).astype(jnp.bfloat16)
        return x_unit, jnp.dot(x_unit, phi_norm, preferred_element_type=jnp.float32)

    def dispatch(inputs):
        x_seq, seq_len = inputs
        x_unit, logits = seq_logits(x_seq)
        valid_mask = (positions < seq_len)[:, None]
        col_max = jnp.max(jnp.where(valid_mask, logits, NEG_BIG), axis=0)
        weights = jnp.where(valid_mask, jnp.exp(logits - col_max[None, :]), 0.0)
        col_sum = jnp.sum(weights, axis=0)
        slot_num = jnp.dot(weights.astype(jnp.bfloat16).T, x_seq, preferred_element_type=jnp.float32)
        return (slot_num / col_sum[:, None]).astype(jnp.bfloat16)

    slot_in = lax.map(dispatch, (x_tokens, lengths))
    expert_in = jnp.transpose(slot_in.reshape(SEQ_BATCH, NUM_EXPERTS, EXPERT_SLOTS, MODEL_DIM), (1, 0, 2, 3)).reshape(NUM_EXPERTS, SEQ_BATCH * EXPERT_SLOTS, MODEL_DIM)

    def expert_ffn(inputs):
        expert_rows, w_first, w_second = inputs
        hidden = jax.nn.gelu(jnp.dot(expert_rows, w_first, preferred_element_type=jnp.float32), approximate=True).astype(jnp.bfloat16)
        return jnp.dot(hidden, w_second, preferred_element_type=jnp.float32).astype(jnp.bfloat16)

    expert_out = lax.map(expert_ffn, (expert_in, w_in, w_out))
    slot_out = jnp.transpose(expert_out.reshape(NUM_EXPERTS, SEQ_BATCH, EXPERT_SLOTS, MODEL_DIM), (1, 0, 2, 3)).reshape(SEQ_BATCH, SLOT_TOTAL, MODEL_DIM)

    def combine(inputs):
        x_seq, slot_seq = inputs
        x_unit, logits = seq_logits(x_seq)
        mix_weights = jax.nn.softmax(logits, axis=-1).astype(jnp.bfloat16)
        moe_part = jnp.dot(mix_weights, slot_seq, preferred_element_type=jnp.float32)
        hid_shared = jax.nn.gelu(jnp.dot(x_unit, ws_in, preferred_element_type=jnp.float32), approximate=True).astype(jnp.bfloat16)
        dense_part = jnp.dot(hid_shared, ws_out, preferred_element_type=jnp.float32)
        return (moe_part + dense_part).astype(jnp.bfloat16)

    return lax.map(combine, (x_tokens, slot_out))
```

```python
import functools

import jax
import jax.numpy as jnp
from jax import lax
from jax.experimental import pallas as pl
from jax.experimental.pallas import tpu as pltpu
from jax.sharding import PartitionSpec as P

NORM_EPS = 1e-6
NEG_BIG = -1e30
F32 = jnp.float32
BF16 = jnp.bfloat16
SUB = 8
NU = 2
NQ = 4


def unit_rows(values, axis_id):
    wide_vals = values.astype(F32)
    return wide_vals / jnp.sqrt(jnp.sum(wide_vals * wide_vals, axis=axis_id, keepdims=True) + NORM_EPS)


def row_unit(x):
    xf = x.astype(F32)
    return (xf * lax.rsqrt(jnp.sum(xf * xf, axis=-1, keepdims=True) + NORM_EPS)).astype(BF16)


def params(sem, vmem_mb):
    return pltpu.CompilerParams(dimension_semantics=sem, vmem_limit_bytes=vmem_mb << 20)


def head_kernel(nb, len_ref, rank_ref, pnt_ref, x_ref, s0, s1, k0, k1, st_ref):
    step = pl.program_id(0)
    tok = x_ref.shape[1]
    slots = pnt_ref.shape[0]
    lane = lax.broadcasted_iota(jnp.int32, (slots, tok), 1)
    base = rank_ref[0] * tok

    @pl.when(step == 0)
    def _():
        st_ref[...] = jnp.zeros_like(st_ref)

    st = st_ref[...]
    stl = lax.broadcasted_iota(jnp.int32, st.shape, 1)
    half = st.shape[1] // 2
    prev = None
    outs = ((s0, s1), (k0, k1))
    for i in range(nb):
        b = step * nb + i
        xb = x_ref[i]
        xn = row_unit(xb)
        lt = lax.dot_general(pnt_ref[...], xn, (((1,), (1,)), ((), ())), preferred_element_type=F32)
        valid = (base + lane) < len_ref[b]
        m = jnp.max(jnp.where(valid, lt, NEG_BIG), axis=1, keepdims=True)
        e = jnp.where(valid, jnp.exp(lt - m), 0.0)
        z = jnp.sum(e, axis=1, keepdims=True)
        num = jnp.dot(e.astype(BF16), xb, preferred_element_type=F32)
        st = jnp.where(stl == b, m, jnp.where(stl == half + b, z, st))
        if i % 2 == 0:
            prev = num
        else:
            for rc in range(2):
                for u in range(NU):
                    for q in range(NQ):
                        r = ((rc * NU + u) * NQ + q) * SUB
                        both = jnp.concatenate([prev[r:r + SUB], num[r:r + SUB]], axis=0)
                        outs[1 - rc][u][q, (i - 1) * SUB:(i + 1) * SUB, :] = both.astype(BF16)
    st_ref[...] = st


def head_call(x_blk, lens, rank, pnt):
    batch, tok, width = x_blk.shape
    slots = pnt.shape[0]
    nb = 4
    rows = batch * SUB
    part = jax.ShapeDtypeStruct((NQ, rows, width), BF16)
    pspec = pl.BlockSpec((NQ, nb * SUB, width), lambda i, *_: (0, i, 0))
    return pl.pallas_call(
        functools.partial(head_kernel, nb),
        grid_spec=pltpu.PrefetchScalarGridSpec(
            num_scalar_prefetch=2,
            grid=(batch // nb,),
            in_specs=[
                pl.BlockSpec((slots, width), lambda i, *_: (0, 0)),
                pl.BlockSpec((nb, tok, width), lambda i, *_: (i, 0, 0)),
            ],
            out_specs=[pspec] * 4 + [pl.BlockSpec((slots, 2 * batch), lambda i, *_: (0, 0))],
        ),
        out_shape=[part] * 4 + [jax.ShapeDtypeStruct((slots, 2 * batch), F32)],
        compiler_params=params(("arbitrary",), 32),
        cost_estimate=pl.CostEstimate(flops=4 * batch * tok * slots * width, bytes_accessed=2 * batch * (tok + slots) * width, transcendentals=batch * tok * slots),
        name="head",
    )(lens, rank, pnt, x_blk)


def merge_kernel(st_ref, keep_ref, recv_ref, out_ref):
    batch = st_ref.shape[2] // 2
    nb = out_ref.shape[0] // SUB
    ms = [st_ref[p][:, :batch] for p in range(4)]
    zs = [st_ref[p][:, batch:] for p in range(4)]
    top = jnp.maximum(jnp.maximum(ms[0], ms[1]), jnp.maximum(ms[2], ms[3]))
    ws = [jnp.exp(m - top) for m in ms]
    total = ws[0] * zs[0] + ws[1] * zs[1] + ws[2] * zs[2] + ws[3] * zs[3]
    inv = 1.0 / total
    w0 = ws[0] * inv
    w1 = ws[1] * inv
    for h in range(batch // nb):

        @pl.when(pl.program_id(0) == h)
        def _(h=h):
            for i in range(0, nb, 2):
                pieces = []
                kk = keep_ref[0, i * SUB:(i + 2) * SUB, :].astype(F32)
                rr = recv_ref[0, i * SUB:(i + 2) * SUB, :].astype(F32)
                for j in range(2):
                    b = h * nb + i + j
                    pieces.append(kk[j * SUB:(j + 1) * SUB] * w0[:, b:b + 1] + rr[j * SUB:(j + 1) * SUB] * w1[:, b:b + 1])
                out_ref[i * SUB:(i + 2) * SUB, :] = jnp.concatenate(pieces, axis=0).astype(BF16)


def merge_call(st, keep, recv, q):
    _, rows, width = keep.shape
    blk = rows // 2
    spec = pl.BlockSpec((1, blk, width), lambda i: (q, i, 0))
    return pl.pallas_call(
        merge_kernel,
        grid=(2,),
        in_specs=[pl.BlockSpec(st.shape, lambda i: (0, 0, 0)), spec, spec],
        out_specs=pl.BlockSpec((blk, width), lambda i: (i, 0)),
        out_shape=jax.ShapeDtypeStruct((rows, width), BF16),
        compiler_params=params(("arbitrary",), 16),
        cost_estimate=pl.CostEstimate(flops=4 * rows * width, bytes_accessed=6 * rows * width, transcendentals=0),
        name="merge",
    )(st, keep, recv)


def gelu(h):
    return jax.nn.gelu(h, approximate=True)


def expert_kernel(nsplit, data_ref, a0, a1, b0, b1, w1_ref, w2_ref, *rest):
    outs = rest[:2 * nsplit]
    s_a, s_b, acc, xs = rest[2 * nsplit:]
    e = pl.program_id(0)
    f = pl.program_id(1)
    nf = pl.num_programs(1)
    batch = s_a.shape[1] // SUB
    lanes = s_a.shape[0]

    @pl.when((e == 0) & (f == 0))
    def _():
        for k in range(lanes):
            cols = slice(k * 128, (k + 1) * 128)
            s_a[k] = a0[:, cols].astype(F32) + a1[:, cols].astype(F32)
            s_b[k] = b0[:, cols].astype(F32) + b1[:, cols].astype(F32)

    @pl.when(f == 0)
    def _():
        for k in range(lanes):
            cols = slice(k * 128, (k + 1) * 128)
            xs[:batch, cols] = s_a[k, pl.ds(e, batch, stride=SUB), :].astype(BF16)
            xs[batch:, cols] = s_b[k, pl.ds(e, batch, stride=SUB), :].astype(BF16)

    h = gelu(jnp.dot(xs[...], w1_ref[0], preferred_element_type=F32)).astype(BF16)
    y = jnp.dot(h, w2_ref[0], preferred_element_type=F32)

    @pl.when(f == 0)
    def _():
        acc[...] = y

    @pl.when(f != 0)
    def _():
        acc[...] += y

    @pl.when(f == nf - 1)
    def _():
        for k in range(lanes):
            cols = slice(k * 128, (k + 1) * 128)
            s_a[k, pl.ds(e, batch, stride=SUB), :] = acc[:batch, cols]
            s_b[k, pl.ds(e, batch, stride=SUB), :] = acc[batch:, cols]

    @pl.when((e == pl.num_programs(0) - 1) & (f == nf - 1))
    def _():
        blk = s_a.shape[1] // nsplit
        for n in range(nsplit):
            for k in range(lanes):
                cols = slice(k * 128, (k + 1) * 128)
                outs[n][:, cols] = s_a[k, n * blk:(n + 1) * blk, :].astype(BF16)
                outs[nsplit + n][:, cols] = s_b[k, n * blk:(n + 1) * blk, :].astype(BF16)


def expert_call(data_rank, a0, a1, b0, b1, w_in, w_out, u, nsplit):
    rows, width = a0.shape
    ff = w_in.shape[2]
    owned = w_in.shape[0] // 2
    nf = 2
    fb = ff // nf
    full = pl.BlockSpec((rows, width), lambda e, f, d: (0, 0))
    out = jax.ShapeDtypeStruct((rows // nsplit, width), BF16)
    ospec = pl.BlockSpec((rows // nsplit, width), lambda e, f, d: (0, 0))
    return pl.pallas_call(
        functools.partial(expert_kernel, nsplit),
        grid_spec=pltpu.PrefetchScalarGridSpec(
            num_scalar_prefetch=1,
            grid=(SUB, nf),
            in_specs=[full] * 4 + [
                pl.BlockSpec((1, width, fb), lambda e, f, d: (d[0] * owned + u * SUB + e, 0, f)),
                pl.BlockSpec((1, fb, width), lambda e, f, d: (d[0] * owned + u * SUB + e, f, 0)),
            ],
            out_specs=[ospec] * (2 * nsplit),
            scratch_shapes=[
                pltpu.VMEM((width // 128, rows, 128), F32),
                pltpu.VMEM((width // 128, rows, 128), F32),
                pltpu.VMEM((2 * rows // SUB, width), F32),
                pltpu.VMEM((2 * rows // SUB, width), BF16),
            ],
        ),
        out_shape=[out] * (2 * nsplit),
        compiler_params=params(("arbitrary", "arbitrary"), 40),
        cost_estimate=pl.CostEstimate(flops=8 * rows * width * ff, bytes_accessed=4 * SUB * width * ff, transcendentals=2 * rows * ff),
        name="experts",
    )(data_rank, a0, a1, b0, b1, w_in, w_out)


def dense_kernel(nf, tok_seq, x_ref, pn_ref, w1_hbm, w2_hbm, y_ref, c_ref, w1, w2, sems):
    step = pl.program_id(0)
    width, ff = w1.shape
    fb = ff // nf

    def copies(j):
        return (
            pltpu.make_async_copy(w1_hbm.at[:, pl.ds(j * fb, fb)], w1.at[:, pl.ds(j * fb, fb)], sems.at[0, j]),
            pltpu.make_async_copy(w2_hbm.at[pl.ds(j * fb, fb), :], w2.at[pl.ds(j * fb, fb), :], sems.at[1, j]),
        )

    @pl.when(step == 0)
    def _():
        for j in range(nf):
            for cp in copies(j):
                cp.start()

    xn = row_unit(x_ref[...])
    logits = jnp.dot(xn, pn_ref[...], preferred_element_type=F32)
    t = lax.broadcasted_iota(jnp.int32, logits.shape, 0)
    s = lax.broadcasted_iota(jnp.int32, logits.shape, 1)
    mine = ((t // tok_seq) % 2) == ((s // SUB) % 2)
    logits = jnp.where(mine, logits, NEG_BIG)
    ex = jnp.exp(logits - jnp.max(logits, axis=1, keepdims=True))
    c_ref[...] = (ex / jnp.sum(ex, axis=1, keepdims=True)).astype(BF16)

    for j in range(nf):

        @pl.when(step == 0)
        def _(j=j):
            for cp in copies(j):
                cp.wait()

        h = gelu(jnp.dot(xn, w1[:, j * fb:(j + 1) * fb], preferred_element_type=F32)).astype(BF16)
        y = jnp.dot(h, w2[j * fb:(j + 1) * fb, :], preferred_element_type=F32)
        if j == 0:
            y_ref[...] = y
        else:
            y_ref[...] += y


def dense_call(x2, pn_pair, ws_in, ws_out, tok_seq, part, nparts):
    tokens, width = x2.shape
    ff = ws_in.shape[1]
    cols = pn_pair.shape[1]
    tile = 512
    nf = 3
    steps = tokens // nparts // tile
    return pl.pallas_call(
        functools.partial(dense_kernel, nf, tok_seq),
        grid=(steps,),
        in_specs=[
            pl.BlockSpec((tile, width), lambda i: (part * steps + i, 0)),
            pl.BlockSpec((width, cols), lambda i: (0, 0)),
            pl.BlockSpec(memory_space=pl.ANY),
            pl.BlockSpec(memory_space=pl.ANY),
        ],
        out_specs=[
            pl.BlockSpec((tile, width), lambda i: (i, 0)),
            pl.BlockSpec((tile, cols), lambda i: (i, 0)),
        ],
        out_shape=[
            jax.ShapeDtypeStruct((tokens // nparts, width), F32),
            jax.ShapeDtypeStruct((tokens // nparts, cols), BF16),
        ],
        scratch_shapes=[
            pltpu.VMEM((width, ff), BF16),
            pltpu.VMEM((ff, width), BF16),
            pltpu.SemaphoreType.DMA((2, nf)),
        ],
        compiler_params=params(("arbitrary",), 48),
        cost_estimate=pl.CostEstimate(flops=4 * tokens // nparts * width * ff, bytes_accessed=6 * tokens // nparts * width + 4 * width * ff, transcendentals=tokens // nparts * ff),
        name=f"dense{part}",
    )(x2, pn_pair, ws_in, ws_out)


def combine_kernel(npair, tok_seq, n_arr, c_ref, y2_ref, *rest):
    arrs, out_ref = rest[:n_arr], rest[n_arr]
    for p in range(npair):
        ys = jnp.concatenate([a[p * 2 * SUB:(p + 1) * 2 * SUB, :] for a in arrs], axis=0)
        r = slice(p * 2 * tok_seq, (p + 1) * 2 * tok_seq)
        y1 = jnp.dot(c_ref[r, :], ys, preferred_element_type=F32)
        out_ref[r, :] = (y1 + y2_ref[r, :]).astype(BF16)


def combine_call(c, y2, arrs, tok_seq, part, nparts):
    tokens, width = y2.shape
    npair = 2
    tile = npair * 2 * tok_seq
    steps = tokens // tile
    rows = npair * 2 * SUB

    def aspec(a):
        off = 0 if a.shape[0] == steps * rows else part * steps
        return pl.BlockSpec((rows, width), lambda i: (off + i, 0))

    return pl.pallas_call(
        functools.partial(combine_kernel, npair, tok_seq, len(arrs)),
        grid=(steps,),
        in_specs=[
            pl.BlockSpec((tile, c.shape[1]), lambda i: (i, 0)),
            pl.BlockSpec((tile, width), lambda i: (i, 0)),
        ] + [aspec(a) for a in arrs],
        out_specs=pl.BlockSpec((tile, width), lambda i: (i, 0)),
        out_shape=jax.ShapeDtypeStruct((tokens, width), BF16),
        compiler_params=params(("arbitrary",), 32),
        cost_estimate=pl.CostEstimate(flops=2 * tokens * width * c.shape[1], bytes_accessed=8 * tokens * width, transcendentals=0),
        name=f"combine{part}",
    )(c, y2, *arrs)


NSPLIT = 2
NDENSE = 2


def solution(mesh):
    nd, ns = mesh.shape['data'], mesh.shape['seq']
    tok_spec = P('data', 'seq', None)
    expert_spec = P('seq', None, None)
    both = ('data', 'seq')
    core_perm = [(i, i ^ 1) for i in range(ns)]
    x_perm = [(i, i ^ 2) for i in range(ns)]
    xc_perm = [(i, i ^ 3) for i in range(ns)]
    y_perm = [(i, i ^ 1) for i in range(nd)]
    diag_perm = [(i, i ^ (ns + 2)) for i in range(nd * ns)]

    def swap_core(v):
        return lax.ppermute(v, 'seq', core_perm)

    def swap_x(v):
        return lax.ppermute(v, 'seq', x_perm)

    def swap_y(v):
        return lax.ppermute(v, 'data', y_perm)

    def swap_diag(v):
        return lax.ppermute(v, both, diag_perm)

    def per_device(x_blk, len_blk, phi_slots, scale_g, w_in, w_out, ws_in, ws_out):
        batch, tok, width = x_blk.shape
        d = lax.axis_index('data').astype(jnp.int32)
        s = lax.axis_index('seq').astype(jnp.int32)
        cb, xb = s % 2, s // 2
        rank = s.reshape(1)
        drank = d.reshape(1)
        pn = (scale_g * unit_rows(phi_slots, 0)).astype(BF16)
        pr = pn.reshape(width, 2, 2, 2, NU, SUB)
        for axis, bit in ((1, xb), (2, cb), (3, d)):
            pr = jnp.where(bit == 1, jnp.flip(pr, axis), pr)
        pr = pr.transpose(0, 2, 4, 1, 3, 5)
        pnt = pr.reshape(width, -1).T
        pn_pair = jnp.broadcast_to(pr.reshape(width, -1, 1, SUB), (width, 2 * NU * NQ, 2, SUB)).reshape(width, -1)

        s0, s1, k0, k1, st = head_call(x_blk, len_blk, rank, pnt)
        send, keep = (s0, s1), (k0, k1)
        st_c, st_x, st_xc = swap_core(st), swap_x(st), lax.ppermute(st, 'seq', xc_perm)
        recv = [swap_core(send[u]) for u in range(NU)]

        def stats(u, q):
            rx, rh = q // 2, q % 2

            def pick(v, rc, rx):
                return v.reshape(2, NU, 2, 2, SUB, 2 * batch)[rc, u, rx, rh]

            return jnp.stack([pick(st, 0, rx), pick(st_c, 1, rx), pick(st_x, 0, 1 - rx), pick(st_xc, 1, 1 - rx)])

        x2 = x_blk.reshape(batch * tok, width)
        got = []
        for u in range(NU):
            part = {q: merge_call(stats(u, q), keep[u], recv[u], q) for q in (3, 2, 1, 0)}
            diag = swap_diag(part[3])
            nbx = swap_x(part[2])
            nby = swap_y(part[1])
            got.append((part[0], nbx, nby, diag))

        dense = [dense_call(x2, pn_pair, ws_in, ws_out, tok, k, NDENSE) for k in range(NDENSE)]

        pieces = {}
        for u in range(NU):
            n = NSPLIT if u == NU - 1 else 1
            ys = expert_call(drank, *got[u], w_in, w_out, u, n)
            for k in range(n):
                mine, other = ys[k], ys[n + k]
                near = [mine, swap_y(other), swap_x(mine), swap_diag(other)]
                for q in range(NQ):
                    pieces[0, u, q, k] = near[q]
                    pieces[1, u, q, k] = swap_core(near[q])

        outs = []
        for k in range(NSPLIT):
            arrs = []
            for rc in range(2):
                for u in range(NU):
                    for q in range(NQ):
                        arrs.append(pieces[rc, u, q, k if u == NU - 1 else 0])
            y2, c = dense[k]
            outs.append(combine_call(c, y2, arrs, tok, k, NSPLIT))
        return jnp.concatenate(outs, axis=0).reshape(batch, tok, width)

    return jax.shard_map(per_device, mesh=mesh, in_specs=(tok_spec, P('data'), P(), P(), expert_spec, expert_spec, P(), P()), out_specs=tok_spec, check_vma=False)
```

```python
import functools
import math

import jax
import jax.numpy as jnp
from jax import lax
from jax.experimental import pallas as pl
from jax.experimental.pallas import tpu as pltpu
from jax.sharding import PartitionSpec as P

NORM_EPS = 1e-6
NEG_BIG = -1e30
F32 = jnp.float32
BF16 = jnp.bfloat16
GELU_A = (2.0 / math.pi) ** 0.5
GELU_B = 0.044715 * GELU_A
SUB = 8
NU = 2
NQ = 4


def unit_rows(values, axis_id):
    wide_vals = values.astype(F32)
    return wide_vals / jnp.sqrt(jnp.sum(wide_vals * wide_vals, axis=axis_id, keepdims=True) + NORM_EPS)


def row_unit(x):
    xf = x.astype(F32)
    return (xf * lax.rsqrt(jnp.sum(xf * xf, axis=-1, keepdims=True) + NORM_EPS)).astype(BF16)


def params(sem, vmem_mb):
    return pltpu.CompilerParams(dimension_semantics=sem, vmem_limit_bytes=vmem_mb << 20)


def head_kernel(nb, len_ref, rank_ref, pnt_ref, x_ref, s0, s1, k0, k1, st_ref):
    step = pl.program_id(0)
    tok = x_ref.shape[1]
    slots = pnt_ref.shape[0]
    lane = lax.broadcasted_iota(jnp.int32, (slots, tok), 1)
    base = rank_ref[0] * tok

    @pl.when(step == 0)
    def _():
        st_ref[...] = jnp.zeros_like(st_ref)

    st = st_ref[...]
    stl = lax.broadcasted_iota(jnp.int32, st.shape, 1)
    half = st.shape[1] // 2
    outs = ((s0, s1), (k0, k1))
    width = x_ref.shape[2]
    x = x_ref[...].reshape(nb * tok, width)
    lts = lax.dot_general(pnt_ref[...], row_unit(x), (((1,), (1,)), ((), ())), preferred_element_type=F32)
    es = []
    for i in range(nb):
        b = step * nb + i
        lt = lts[:, i * tok:(i + 1) * tok]
        valid = (base + lane) < len_ref[b]
        m = jnp.max(jnp.where(valid, lt, NEG_BIG), axis=1, keepdims=True)
        e = jnp.where(valid, jnp.exp(lt - m), 0.0)
        z = jnp.sum(e, axis=1, keepdims=True)
        st = jnp.where(stl == b, m, jnp.where(stl == half + b, z, st))
        es.append(e.astype(BF16))
    nums = [jnp.dot(es[i], x[i * tok:(i + 1) * tok], preferred_element_type=F32) for i in range(nb)]
    for i in range(0, nb, 2):
        for rc in range(2):
            for u in range(NU):
                for q in range(NQ):
                    r = ((rc * NU + u) * NQ + q) * SUB
                    both = jnp.concatenate([nums[i][r:r + SUB], nums[i + 1][r:r + SUB]], axis=0)
                    outs[1 - rc][u][q, i * SUB:(i + 2) * SUB, :] = both.astype(BF16)
    st_ref[...] = st


def head_call(x_blk, lens, rank, pnt):
    batch, tok, width = x_blk.shape
    slots = pnt.shape[0]
    nb = 4
    rows = batch * SUB
    part = jax.ShapeDtypeStruct((NQ, rows, width), BF16)
    pspec = pl.BlockSpec((NQ, nb * SUB, width), lambda i, *_: (0, i, 0))
    return pl.pallas_call(
        functools.partial(head_kernel, nb),
        grid_spec=pltpu.PrefetchScalarGridSpec(
            num_scalar_prefetch=2,
            grid=(batch // nb,),
            in_specs=[
                pl.BlockSpec((slots, width), lambda i, *_: (0, 0)),
                pl.BlockSpec((nb, tok, width), lambda i, *_: (i, 0, 0)),
            ],
            out_specs=[pspec] * 4 + [pl.BlockSpec((slots, 2 * batch), lambda i, *_: (0, 0))],
        ),
        out_shape=[part] * 4 + [jax.ShapeDtypeStruct((slots, 2 * batch), F32)],
        compiler_params=params(("arbitrary",), 60),
        cost_estimate=pl.CostEstimate(flops=4 * batch * tok * slots * width, bytes_accessed=2 * batch * (tok + slots) * width, transcendentals=batch * tok * slots),
        name="head",
    )(lens, rank, pnt, x_blk)


def stat_row(rc, u, q):
    return ((rc * NU + u) * NQ + q) * SUB


def merge_kernel(u, q, st, st_c, st_x, st_xc, keep_ref, recv_ref, *rest):
    out_ref = rest[-1]
    batch = st.shape[1] // 2
    nb = out_ref.shape[0] // SUB
    peers = ((st, 0, q), (st_c, 1, q), (st_x, 0, q ^ 2), (st_xc, 1, q ^ 2))
    rows = [ref[stat_row(rc, u, qq):stat_row(rc, u, qq) + SUB, :] for ref, rc, qq in peers]
    ms = [r[:, :batch] for r in rows]
    zs = [r[:, batch:] for r in rows]
    top = jnp.maximum(jnp.maximum(ms[0], ms[1]), jnp.maximum(ms[2], ms[3]))
    ws = [jnp.exp(m - top) for m in ms]
    total = ws[0] * zs[0] + ws[1] * zs[1] + ws[2] * zs[2] + ws[3] * zs[3]
    inv = 1.0 / total
    w0 = ws[0] * inv
    w1 = ws[1] * inv
    for h in range(batch // nb):

        @pl.when(pl.program_id(0) == h)
        def _(h=h):
            for i in range(0, nb, 2):
                pieces = []
                kk = keep_ref[0, i * SUB:(i + 2) * SUB, :].astype(F32)
                rr = recv_ref[0, i * SUB:(i + 2) * SUB, :].astype(F32)
                for j in range(2):
                    b = h * nb + i + j
                    pieces.append(kk[j * SUB:(j + 1) * SUB] * w0[:, b:b + 1] + rr[j * SUB:(j + 1) * SUB] * w1[:, b:b + 1])
                out_ref[i * SUB:(i + 2) * SUB, :] = jnp.concatenate(pieces, axis=0).astype(BF16)


def merge_call(stats, keep, recv, u, q, after):
    _, rows, width = keep.shape
    blk = rows // 2
    spec = pl.BlockSpec((1, blk, width), lambda i: (q, i, 0))
    return pl.pallas_call(
        functools.partial(merge_kernel, u, q),
        grid=(2,),
        in_specs=[pl.BlockSpec(stats[0].shape, lambda i: (0, 0))] * 4 + [spec, spec] + [pl.BlockSpec(memory_space=pl.ANY)] * len(after),
        out_specs=pl.BlockSpec((blk, width), lambda i: (i, 0)),
        out_shape=jax.ShapeDtypeStruct((rows, width), BF16),
        compiler_params=params(("arbitrary",), 60),
        cost_estimate=pl.CostEstimate(flops=4 * rows * width, bytes_accessed=6 * rows * width, transcendentals=0),
        name="merge",
    )(*stats, keep, recv, *after)


def gelu(h):
    return h * (0.5 + 0.5 * jnp.tanh(h * (GELU_A + GELU_B * (h * h))))


def expert_kernel(nsplit, nc, data_ref, a0, a1, b0, b1, w1_ref, w2_ref, after, *rest):
    del after
    outs = rest[:2 * nsplit]
    s_a, s_b, acc, xs = rest[2 * nsplit:]
    e = pl.program_id(0)
    f = pl.program_id(1)
    nf = pl.num_programs(1)
    batch = s_a.shape[1] // SUB
    lanes = s_a.shape[0]

    @pl.when((e == 0) & (f == 0))
    def _():
        for k in range(lanes):
            cols = slice(k * 128, (k + 1) * 128)
            s_a[k] = a0[:, cols].astype(F32) + a1[:, cols].astype(F32)
            s_b[k] = b0[:, cols].astype(F32) + b1[:, cols].astype(F32)

    @pl.when(f == 0)
    def _():
        for k in range(lanes):
            cols = slice(k * 128, (k + 1) * 128)
            xs[:batch, cols] = s_a[k, pl.ds(e, batch, stride=SUB), :].astype(BF16)
            xs[batch:, cols] = s_b[k, pl.ds(e, batch, stride=SUB), :].astype(BF16)

    fb = w1_ref.shape[2] // nc
    xv = xs[...]

    def up(j):
        return jnp.dot(xv, w1_ref[0, :, j * fb:(j + 1) * fb], preferred_element_type=F32)

    y = None
    h = up(0)
    for j in range(nc):
        nxt = up(j + 1) if j + 1 < nc else None
        t = jnp.dot(gelu(h).astype(BF16), w2_ref[0, j * fb:(j + 1) * fb, :], preferred_element_type=F32)
        y = t if y is None else y + t
        h = nxt

    @pl.when(f == 0)
    def _():
        acc[...] = y

    @pl.when(f != 0)
    def _():
        acc[...] += y

    @pl.when(f == nf - 1)
    def _():
        for k in range(lanes):
            cols = slice(k * 128, (k + 1) * 128)
            s_a[k, pl.ds(e, batch, stride=SUB), :] = acc[:batch, cols]
            s_b[k, pl.ds(e, batch, stride=SUB), :] = acc[batch:, cols]

    @pl.when((e == pl.num_programs(0) - 1) & (f == nf - 1))
    def _():
        blk = s_a.shape[1] // nsplit
        for n in range(nsplit):
            for k in range(lanes):
                cols = slice(k * 128, (k + 1) * 128)
                outs[n][:, cols] = s_a[k, n * blk:(n + 1) * blk, :].astype(BF16)
                outs[nsplit + n][:, cols] = s_b[k, n * blk:(n + 1) * blk, :].astype(BF16)


def expert_call(data_rank, a0, a1, b0, b1, w_in, w_out, u, nsplit, after, nf=2, nc=3):
    rows, width = a0.shape
    ff = w_in.shape[2]
    owned = w_in.shape[0] // 2
    fb = ff // nf
    full = pl.BlockSpec((rows, width), lambda e, f, d: (0, 0))
    out = jax.ShapeDtypeStruct((rows // nsplit, width), BF16)
    ospec = pl.BlockSpec((rows // nsplit, width), lambda e, f, d: (0, 0))
    return pl.pallas_call(
        functools.partial(expert_kernel, nsplit, nc),
        grid_spec=pltpu.PrefetchScalarGridSpec(
            num_scalar_prefetch=1,
            grid=(SUB, nf),
            in_specs=[full] * 4 + [
                pl.BlockSpec((1, width, fb), lambda e, f, d: (d[0] * owned + u * SUB + e, 0, f)),
                pl.BlockSpec((1, fb, width), lambda e, f, d: (d[0] * owned + u * SUB + e, f, 0)),
                pl.BlockSpec(memory_space=pl.ANY),
            ],
            out_specs=[ospec] * (2 * nsplit),
            scratch_shapes=[
                pltpu.VMEM((width // 128, rows, 128), F32),
                pltpu.VMEM((width // 128, rows, 128), F32),
                pltpu.VMEM((2 * rows // SUB, width), F32),
                pltpu.VMEM((2 * rows // SUB, width), BF16),
            ],
        ),
        out_shape=[out] * (2 * nsplit),
        compiler_params=params(("arbitrary", "arbitrary"), 60),
        cost_estimate=pl.CostEstimate(flops=8 * rows * width * ff, bytes_accessed=4 * SUB * width * ff, transcendentals=2 * rows * ff),
        name="experts",
    )(data_rank, a0, a1, b0, b1, w_in, w_out, after)


def dense_kernel(nf, tok_seq, x_ref, pn_ref, w1_hbm, w2_hbm, y_ref, c_ref, w1, w2, sems):
    step = pl.program_id(0)
    _, ff = w1.shape
    fb = ff // nf

    def copies(j):
        return (
            pltpu.make_async_copy(w1_hbm.at[:, pl.ds(j * fb, fb)], w1.at[:, pl.ds(j * fb, fb)], sems.at[0, j]),
            pltpu.make_async_copy(w2_hbm.at[pl.ds(j * fb, fb), :], w2.at[pl.ds(j * fb, fb), :], sems.at[1, j]),
        )

    def body(first):
        if first:
            for j in range(nf):
                for cp in copies(j):
                    cp.start()
        xn = row_unit(x_ref[...])
        logits = jnp.dot(xn, pn_ref[...], preferred_element_type=F32)
        t = lax.broadcasted_iota(jnp.int32, logits.shape, 0)
        s = lax.broadcasted_iota(jnp.int32, logits.shape, 1)
        mine = ((t // tok_seq) % 2) == ((s // SUB) % 2)
        logits = jnp.where(mine, logits, NEG_BIG)
        ex = jnp.exp(logits - jnp.max(logits, axis=1, keepdims=True))
        c_ref[...] = (ex / jnp.sum(ex, axis=1, keepdims=True)).astype(BF16)
        if first:
            for j in range(nf):
                up_copy, down_copy = copies(j)
                up_copy.wait()
                h = gelu(jnp.dot(xn, w1[:, j * fb:(j + 1) * fb], preferred_element_type=F32)).astype(BF16)
                down_copy.wait()
                y = jnp.dot(h, w2[j * fb:(j + 1) * fb, :], preferred_element_type=F32)
                if j == 0:
                    y_ref[...] = y
                else:
                    y_ref[...] += y
        else:
            h = gelu(jnp.dot(xn, w1[...], preferred_element_type=F32)).astype(BF16)
            y_ref[...] = jnp.dot(h, w2[...], preferred_element_type=F32)

    @pl.when(step == 0)
    def _():
        body(True)

    @pl.when(step > 0)
    def _():
        body(False)


def dense_call(x2, pn_pair, ws_in, ws_out, tok_seq, first, count, prev, after):
    tokens, width = x2.shape
    ff = ws_in.shape[1]
    cols = pn_pair.shape[1]
    tile = 512
    nf = 3
    hbm = pl.BlockSpec(memory_space=pl.ANY)
    extra = list(prev) + list(after)

    def kernel(x_ref, pn_ref, w1_hbm, w2_hbm, *rest):
        dense_kernel(nf, tok_seq, x_ref, pn_ref, w1_hbm, w2_hbm, *rest[len(extra):])

    return pl.pallas_call(
        kernel,
        grid=(count,),
        in_specs=[
            pl.BlockSpec((tile, width), lambda i: (first + i, 0)),
            pl.BlockSpec((width, cols), lambda i: (0, 0)),
            hbm,
            hbm,
        ] + [hbm] * len(extra),
        out_specs=[
            pl.BlockSpec((tile, width), lambda i: (first + i, 0)),
            pl.BlockSpec((tile, cols), lambda i: (first + i, 0)),
        ],
        out_shape=[
            jax.ShapeDtypeStruct((tokens, width), F32),
            jax.ShapeDtypeStruct((tokens, cols), BF16),
        ],
        input_output_aliases={4: 0, 5: 1} if prev else {},
        scratch_shapes=[
            pltpu.VMEM((width, ff), BF16),
            pltpu.VMEM((ff, width), BF16),
            pltpu.SemaphoreType.DMA((2, nf)),
        ],
        compiler_params=params(("arbitrary",), 60),
        cost_estimate=pl.CostEstimate(flops=4 * count * tile * width * ff, bytes_accessed=6 * count * tile * width + 4 * width * ff, transcendentals=count * tile * ff),
    )(x2, pn_pair, ws_in, ws_out, *extra)


def combine_kernel(npair, tok_seq, n_arr, c_ref, y2_ref, *rest):
    arrs, out_ref = rest[:n_arr], rest[n_arr]
    for p in range(npair):
        ys = jnp.concatenate([a[p * 2 * SUB:(p + 1) * 2 * SUB, :] for a in arrs], axis=0)
        r = slice(p * 2 * tok_seq, (p + 1) * 2 * tok_seq)
        y1 = jnp.dot(c_ref[r, :], ys, preferred_element_type=F32)
        out_ref[r, :] = (y1 + y2_ref[r, :]).astype(BF16)


def combine_call(c, y2, arrs, tok_seq):
    tokens, width = y2.shape
    npair = 2
    tile = npair * 2 * tok_seq
    rows = npair * 2 * SUB
    return pl.pallas_call(
        functools.partial(combine_kernel, npair, tok_seq, len(arrs)),
        grid=(tokens // tile,),
        in_specs=[
            pl.BlockSpec((tile, c.shape[1]), lambda i: (i, 0)),
            pl.BlockSpec((tile, width), lambda i: (i, 0)),
        ] + [pl.BlockSpec((rows, width), lambda i: (i, 0))] * len(arrs),
        out_specs=pl.BlockSpec((tile, width), lambda i: (i, 0)),
        out_shape=jax.ShapeDtypeStruct((tokens, width), BF16),
        compiler_params=params(("arbitrary",), 60),
        cost_estimate=pl.CostEstimate(flops=2 * tokens * width * c.shape[1], bytes_accessed=8 * tokens * width, transcendentals=0),
        name="combine",
    )(c, y2, *arrs)


DENSE = ((0, 5), (5, 2), (7, 6), (13, 3))


def solution(mesh):
    nd, ns = mesh.shape['data'], mesh.shape['seq']
    tok_spec = P('data', 'seq', None)
    expert_spec = P('seq', None, None)
    both = ('data', 'seq')
    core_perm = [(i, i ^ 1) for i in range(ns)]
    x_perm = [(i, i ^ 2) for i in range(ns)]
    xc_perm = [(i, i ^ 3) for i in range(ns)]
    y_perm = [(i, i ^ 1) for i in range(nd)]
    diag_perm = [(i, i ^ (ns + 2)) for i in range(nd * ns)]

    def swap_core(v):
        return lax.ppermute(v, 'seq', core_perm)

    def swap_x(v):
        return lax.ppermute(v, 'seq', x_perm)

    def swap_y(v):
        return lax.ppermute(v, 'data', y_perm)

    def swap_diag(v):
        return lax.ppermute(v, both, diag_perm)

    def layer(x_blk, len_blk, phi_slots, scale_g, w_in, w_out, ws_in, ws_out):
        batch, tok, width = x_blk.shape
        d = lax.axis_index('data').astype(jnp.int32)
        s = lax.axis_index('seq').astype(jnp.int32)
        cb, xb = s % 2, s // 2
        rank = s.reshape(1)
        drank = d.reshape(1)
        pn = (scale_g * unit_rows(phi_slots, 0)).astype(BF16)
        pr = pn.reshape(width, 2, 2, 2, NU, SUB)
        for axis, bit in ((1, xb), (2, cb), (3, d)):
            pr = jnp.where(bit == 1, jnp.flip(pr, axis), pr)
        pr = pr.transpose(0, 2, 4, 1, 3, 5)
        pnt = pr.reshape(width, -1).T
        pn_pair = jnp.broadcast_to(pr.reshape(width, -1, 1, SUB), (width, 2 * NU * NQ, 2, SUB)).reshape(width, -1)

        s0, s1, k0, k1, st = head_call(x_blk, len_blk, rank, pnt)
        send, keep = (s0, s1), (k0, k1)
        st_c, st_x, st_xc = swap_core(st), swap_x(st), lax.ppermute(st, 'seq', xc_perm)
        recv = [swap_core(send[u]) for u in range(NU)]

        stats = (st, st_c, st_x, st_xc)
        x2 = x_blk.reshape(batch * tok, width)
        got = []
        last = ()
        for u in range(NU):
            part = {}
            for q in (3, 2, 1, 0):
                part[q] = merge_call(stats, keep[u], recv[u], u, q, last)
                last = (part[q],)
            diag = swap_diag(part[3])
            nbx = swap_x(part[2])
            nby = swap_y(part[1])
            got.append((part[0], nbx, nby, diag))

        def dense(k, prev, after):
            return dense_call(x2, pn_pair, ws_in, ws_out, tok, *DENSE[k], prev, after)

        def experts(u, after):
            mine, other = expert_call(drank, *got[u], w_in, w_out, u, 1, after)
            return [mine, swap_y(other), swap_x(mine), swap_diag(other)]

        yc = dense(0, (), (got[1][0],))
        near0 = experts(0, yc[1])
        yc = dense(1, yc, (near0[0],))
        near1 = experts(1, yc[1])
        yc = dense(2, yc, (near1[0],))
        far0 = [swap_core(v) for v in near0]
        far1 = [swap_core(v) for v in near1]
        y2, c = dense(3, yc, ())
        return combine_call(c, y2, near0 + near1 + far0 + far1, tok).reshape(batch, tok, width)

    return jax.shard_map(layer, mesh=mesh, in_specs=(tok_spec, P('data'), P(), P(), expert_spec, expert_spec, P(), P()), out_specs=tok_spec, check_vma=False)
```

```python
import functools
import math

import jax
import jax.numpy as jnp
from jax import lax
from jax.experimental import pallas as pl
from jax.experimental.pallas import tpu as pltpu
from jax.sharding import PartitionSpec as P

NORM_EPS = 1e-6
NEG_BIG = -1e30
F32 = jnp.float32
BF16 = jnp.bfloat16
GELU_A = (2.0 / math.pi) ** 0.5
GELU_B = 0.044715 * GELU_A
SUB = 8
NU = 2
NQ = 4


def unit_rows(values, axis_id):
    wide_vals = values.astype(F32)
    return wide_vals / jnp.sqrt(jnp.sum(wide_vals * wide_vals, axis=axis_id, keepdims=True) + NORM_EPS)


def row_unit(x):
    xf = x.astype(F32)
    return (xf * lax.rsqrt(jnp.sum(xf * xf, axis=-1, keepdims=True) + NORM_EPS)).astype(BF16)


def params(sem, vmem_mb):
    return pltpu.CompilerParams(dimension_semantics=sem, vmem_limit_bytes=vmem_mb << 20)


def gelu(h):
    return h * (0.5 + 0.5 * jnp.tanh(h * (GELU_A + GELU_B * (h * h))))


HEAD = 16
D_A, D_B, D_C = 5, 2, 9
T_E0 = HEAD + D_A
T_DB = T_E0 + SUB
T_E1 = T_DB + D_B
T_DC = T_E1 + SUB
STEPS = T_DC + D_C
T_FWD = T_DC + 4
RING = 4
WSLOT = 3


def pick(t, head, e0, e1):
    late = jnp.where(t < T_E1, t - HEAD - SUB, jnp.where(t < T_DC, e1, t - HEAD - 2 * SUB))
    early = jnp.where(t < T_E0, t - HEAD, jnp.where(t < T_DB, e0, late))
    return jnp.where(t < HEAD, head, early)


def x_tile(t):
    return pick(t, t, D_A, D_A + D_B)


def out_tile(t):
    return pick(t, 0, D_A - 1, D_A + D_B - 1)


def ys_index(rc, u, q):
    return (rc * NU + u) * NQ + q


def step_kernel(
    tok, len_ref, pnt_ref, pn_ref, x_ref, ws1_hbm, ws2_hbm, w1_hbm, w2_hbm,
    y2_ref, c_ref, ys_ref,
    ring, keep, recv, drecv, st, st_in, w1, w2, ew1, ew2, s_a, s_b, xs,
    ring_send, p_recv, st_send, st_recv, d_send, d_recv, r_send, r_recv, own_sem, f_send, f_recv, w_sem, e_sem,
):
    t = pl.program_id(0)
    d = lax.axis_index('data')
    s = lax.axis_index('seq')
    core = s + 1 - 2 * (s % 2)
    owned = w1_hbm.shape[0] // 2
    ff = w1.shape[1]
    half_ff = ff // 2
    nb = x_ref.shape[0] // tok
    slots = pnt_ref.shape[0]
    batch = HEAD * nb
    rows = nb * SUB
    lanes = s_a.shape[0]

    def peer(rx, rh):
        return (d + rh * (1 - 2 * d), (s + 2 * rx) % 4)

    def remote(src, dst, send, rec, dev):
        return pltpu.make_async_remote_copy(src_ref=src, dst_ref=dst, send_sem=send, recv_sem=rec, device_id=dev, device_id_type=pl.DeviceIdType.MESH)

    def p_copy(i):
        return remote(ring.at[i % RING], recv.at[i], ring_send.at[i % RING], p_recv.at[i], (d, core))

    def st_copy(k):
        return remote(st, st_in.at[k], st_send.at[k], st_recv.at[k], (d, (core, (s + 2) % 4, 3 - s)[k]))

    def d_copy(u, q):
        return remote(keep.at[:, u, q], drecv.at[u, q - 1], d_send.at[u, q - 1], d_recv.at[u, q - 1], peer(q // 2, q % 2))

    def r_copy(u, q):
        return remote(recv.at[:, u, q % 2], ys_ref.at[ys_index(0, u, q)], r_send.at[u, q - 1], r_recv.at[u, q - 1], peer(q // 2, q % 2))

    def own_copy(u):
        return pltpu.make_async_copy(recv.at[:, u, 0], ys_ref.at[ys_index(0, u, 0)], own_sem.at[u])

    def f_copy(u, q):
        src = recv.at[:, u, 0] if q == 0 else ys_ref.at[ys_index(0, u, q)]
        return remote(src, ys_ref.at[ys_index(1, u, q)], f_send.at[u, q], f_recv.at[u, q], (d, core))

    def w_copies():
        return (pltpu.make_async_copy(ws1_hbm, w1, w_sem.at[0]), pltpu.make_async_copy(ws2_hbm, w2, w_sem.at[1]))

    def e_copies(n):
        e = d * owned + n // 2
        cols = pl.ds(pl.multiple_of((n % 2) * half_ff, 128), half_ff)
        k = n % WSLOT
        return (
            pltpu.make_async_copy(w1_hbm.at[e, :, cols], ew1.at[k], e_sem.at[0, k]),
            pltpu.make_async_copy(w2_hbm.at[e, cols, :], ew2.at[k], e_sem.at[1, k]),
        )

    @pl.when(t == 0)
    def _():
        barrier = pltpu.get_barrier_semaphore()
        for dev in ((d, core), (d, (s + 2) % 4), (d, 3 - s), peer(0, 1), peer(1, 1)):
            pl.semaphore_signal(barrier, inc=1, device_id=dev, device_id_type=pl.DeviceIdType.MESH)
        pl.semaphore_wait(barrier, 5)
        st[...] = jnp.zeros_like(st)

    @pl.when(t == 1)
    def _():
        for cp in w_copies():
            cp.start()

    @pl.when((t > 0) & (t <= HEAD))
    def _():
        p_copy(t - 1).start()

    @pl.when(t < HEAD)
    def _():
        @pl.when(t >= RING)
        def _():
            p_copy(t - RING).wait_send()

        lane = lax.broadcasted_iota(jnp.int32, (slots, tok), 1)
        base = s * tok
        stv = st[...]
        stl = lax.broadcasted_iota(jnp.int32, stv.shape, 1)
        x = x_ref[...]
        lts = lax.dot_general(pnt_ref[...], row_unit(x), (((1,), (1,)), ((), ())), preferred_element_type=F32)
        es = []
        for i in range(nb):
            b = t * nb + i
            lt = lts[:, i * tok:(i + 1) * tok]
            valid = (base + lane) < len_ref[b]
            m = jnp.max(jnp.where(valid, lt, NEG_BIG), axis=1, keepdims=True)
            e = jnp.where(valid, jnp.exp(lt - m), 0.0)
            z = jnp.sum(e, axis=1, keepdims=True)
            stv = jnp.where(stl == b, m, jnp.where(stl == batch + b, z, stv))
            es.append(e.astype(BF16))
        nums = [jnp.dot(es[i], x[i * tok:(i + 1) * tok], preferred_element_type=F32) for i in range(nb)]
        for i in range(0, nb, 2):
            for u in range(NU):
                for q in range(NQ):
                    for rc in range(2):
                        r = ys_index(rc, u, q) * SUB
                        pair = jnp.concatenate([nums[i][r:r + SUB], nums[i + 1][r:r + SUB]], axis=0).astype(BF16)
                        if rc == 0:
                            keep[t, u, q, i * SUB:(i + 2) * SUB, :] = pair
                        else:
                            ring[t % RING, u, q, i * SUB:(i + 2) * SUB, :] = pair
        st[...] = stv

    @pl.when(t == HEAD)
    def _():
        for k in range(3):
            st_copy(k).start()
        for n in range(WSLOT):
            for cp in e_copies(n):
                cp.start()
        for cp in w_copies():
            cp.wait()
        for k in range(3):
            st_copy(k).wait()
        for i in range(HEAD):
            p_copy(i).wait_recv()
        for i in range(HEAD - RING, HEAD):
            p_copy(i).wait_send()

    def merge(u):
        @pl.loop(0, NQ)
        def _(n):
            q = NQ - 1 - n
            qx = (q + 2) % 4

            def stat(ref, rc, qq):
                return ref[pl.ds(pl.multiple_of(ys_index(rc, u, qq) * SUB, SUB), SUB), :]

            peers = (stat(st, 0, q), stat(st_in.at[0], 1, q), stat(st_in.at[1], 0, qx), stat(st_in.at[2], 1, qx))
            ms = [r[:, :batch] for r in peers]
            zs = [r[:, batch:] for r in peers]
            top = jnp.maximum(jnp.maximum(ms[0], ms[1]), jnp.maximum(ms[2], ms[3]))
            ws = [jnp.exp(m - top) for m in ms]
            inv = 1.0 / (ws[0] * zs[0] + ws[1] * zs[1] + ws[2] * zs[2] + ws[3] * zs[3])
            wk = ws[0] * inv
            wr = ws[1] * inv
            for i in range(HEAD):
                for j in range(0, nb, 2):
                    r = slice(j * SUB, (j + 2) * SUB)
                    kk = keep[i, u, q, r, :].astype(F32)
                    rr = recv[i, u, q, r, :].astype(F32)
                    both = []
                    for o in range(2):
                        b = i * nb + j + o
                        ro = slice(o * SUB, (o + 1) * SUB)
                        both.append(kk[ro] * wk[:, b:b + 1] + rr[ro] * wr[:, b:b + 1])
                    keep[i, u, q, r, :] = jnp.concatenate(both, axis=0).astype(BF16)

            @pl.when(n > 0)
            def _():
                d_copy(u, q + 1).start()

    @pl.when(t == HEAD)
    def _():
        merge(0)

    @pl.when(t == HEAD + 1)
    def _():
        merge(1)

    def unpack(u):
        for q in (1, 2, 3):
            d_copy(u, q).wait_recv()

        @pl.loop(0, HEAD)
        def _(i):
            r = pl.ds(pl.multiple_of(i * rows, rows), rows)
            a = keep[i, u, 0].astype(F32) + drecv[u, 1, i].astype(F32)
            b = drecv[u, 0, i].astype(F32) + drecv[u, 2, i].astype(F32)
            for k in range(lanes):
                s_a[k, r, :] = a[:, k * 128:(k + 1) * 128]
                s_b[k, r, :] = b[:, k * 128:(k + 1) * 128]

    def pack(u):
        @pl.loop(0, HEAD)
        def _(i):
            r = pl.ds(pl.multiple_of(i * rows, rows), rows)
            for k in range(lanes):
                cols = slice(k * 128, (k + 1) * 128)
                recv[i, u, 0, :, cols] = s_a[k, r, :].astype(BF16)
                recv[i, u, 1, :, cols] = s_b[k, r, :].astype(BF16)

    @pl.when(t == T_E0)
    def _():
        unpack(0)

    @pl.when(t == T_E1)
    def _():
        unpack(1)

    is_e = ((t >= T_E0) & (t < T_DB)) | ((t >= T_E1) & (t < T_DC))

    @pl.when(is_e)
    def _():
        k_all = jnp.where(t < T_DB, t - T_E0, t - T_E1 + SUB)
        e = k_all % SUB
        for k in range(lanes):
            cols = slice(k * 128, (k + 1) * 128)
            xs[:batch, cols] = s_a[k, pl.ds(e, batch, stride=SUB), :].astype(BF16)
            xs[batch:, cols] = s_b[k, pl.ds(e, batch, stride=SUB), :].astype(BF16)

        def half(n):
            for cp in e_copies(n):
                cp.wait()
            k = n % WSLOT
            xv = xs[...]
            nc = 3
            fb = half_ff // nc

            def up(j):
                return jnp.dot(xv, ew1[k, :, j * fb:(j + 1) * fb], preferred_element_type=F32)

            y = None
            h = up(0)
            for j in range(nc):
                nxt = up(j + 1) if j + 1 < nc else None
                v = jnp.dot(gelu(h).astype(BF16), ew2[k, j * fb:(j + 1) * fb, :], preferred_element_type=F32)
                y = v if y is None else y + v
                h = nxt

            for k in range(lanes):
                cols = slice(k * 128, (k + 1) * 128)
                pa = pl.ds(e, batch, stride=SUB)

                @pl.when(n % 2 == 0)
                def _(k=k, cols=cols):
                    s_a[k, pa, :] = y[:batch, cols]
                    s_b[k, pa, :] = y[batch:, cols]

                @pl.when(n % 2 == 1)
                def _(k=k, cols=cols):
                    s_a[k, pa, :] += y[:batch, cols]
                    s_b[k, pa, :] += y[batch:, cols]

            @pl.when(n + WSLOT < 2 * owned)
            def _():
                for cp in e_copies(n + WSLOT):
                    cp.start()

        @pl.loop(0, 2)
        def _(hh):
            half(2 * k_all + hh)

    def give(u):
        pack(u)

    @pl.when(t == T_DB - 1)
    def _():
        give(0)

    @pl.when(t == T_DC - 1)
    def _():
        give(1)

    def send_back(u):
        for q in (3, 2, 1):
            r_copy(u, q).start()
        own_copy(u).start()
        f_copy(u, 0).start()

    @pl.when(t == T_DB)
    def _():
        send_back(0)

    @pl.when(t == T_DC)
    def _():
        send_back(1)

    def forward(u):
        for q in (1, 2, 3):
            r_copy(u, q).wait_recv()
            f_copy(u, q).start()

    @pl.when(t == T_FWD)
    def _():
        forward(0)

    @pl.when((t >= HEAD) & jnp.logical_not(is_e))
    def _():
        xn = row_unit(x_ref[...])
        logits = jnp.dot(xn, pn_ref[...], preferred_element_type=F32)
        ti = lax.broadcasted_iota(jnp.int32, logits.shape, 0)
        si = lax.broadcasted_iota(jnp.int32, logits.shape, 1)
        mine = ((ti // tok) % 2) == ((si // SUB) % 2)
        logits = jnp.where(mine, logits, NEG_BIG)
        ex = jnp.exp(logits - jnp.max(logits, axis=1, keepdims=True))
        c_ref[...] = (ex / jnp.sum(ex, axis=1, keepdims=True)).astype(BF16)
        nf = 3
        fb = ff // nf

        def up(j):
            return jnp.dot(xn, w1[:, j * fb:(j + 1) * fb], preferred_element_type=F32)

        h = up(0)
        for j in range(nf):
            nxt = up(j + 1) if j + 1 < nf else None
            y = jnp.dot(gelu(h).astype(BF16), w2[j * fb:(j + 1) * fb, :], preferred_element_type=F32)
            if j == 0:
                y2_ref[...] = y
            else:
                y2_ref[...] += y
            h = nxt

    @pl.when(t == STEPS - 1)
    def _():
        forward(1)
        for u in range(NU):
            own_copy(u).wait()
            for q in (1, 2, 3):
                d_copy(u, q).wait_send()
                r_copy(u, q).wait_send()
            for q in range(NQ):
                f_copy(u, q).wait()


def step_call(lens, pnt, pn_pair, x2, ws_in, ws_out, w_in, w_out, tok):
    tokens, width = x2.shape
    ff = ws_in.shape[1]
    cols = pn_pair.shape[1]
    slots = pnt.shape[0]
    tile = tokens // HEAD
    nb = tile // tok
    rows = nb * SUB
    batch = HEAD * nb
    hbm = pl.BlockSpec(memory_space=pl.ANY)
    dma = pltpu.SemaphoreType.DMA
    return pl.pallas_call(
        functools.partial(step_kernel, tok),
        grid=(STEPS,),
        in_specs=[
            pl.BlockSpec(memory_space=pltpu.SMEM),
            pl.BlockSpec((slots, width), lambda t: (0, 0)),
            pl.BlockSpec((width, cols), lambda t: (0, 0)),
            pl.BlockSpec((tile, width), lambda t: (x_tile(t), 0)),
            hbm, hbm, hbm, hbm,
        ],
        out_specs=[
            pl.BlockSpec((tile, width), lambda t: (out_tile(t), 0)),
            pl.BlockSpec((tile, cols), lambda t: (out_tile(t), 0)),
            hbm,
        ],
        out_shape=[
            jax.ShapeDtypeStruct((tokens, width), F32),
            jax.ShapeDtypeStruct((tokens, cols), BF16),
            jax.ShapeDtypeStruct((2 * NU * NQ, HEAD, rows, width), BF16),
        ],
        scratch_shapes=[
            pltpu.VMEM((RING, NU, NQ, rows, width), BF16),
            pltpu.VMEM((HEAD, NU, NQ, rows, width), BF16),
            pltpu.VMEM((HEAD, NU, NQ, rows, width), BF16),
            pltpu.VMEM((NU, 3, HEAD, rows, width), BF16),
            pltpu.VMEM((slots, 2 * batch), F32),
            pltpu.VMEM((3, slots, 2 * batch), F32),
            pltpu.VMEM((width, ff), BF16),
            pltpu.VMEM((ff, width), BF16),
            pltpu.VMEM((WSLOT, width, ff // 2), BF16),
            pltpu.VMEM((WSLOT, ff // 2, width), BF16),
            pltpu.VMEM((width // 128, batch * SUB, 128), F32),
            pltpu.VMEM((width // 128, batch * SUB, 128), F32),
            pltpu.VMEM((2 * batch, width), BF16),
            dma((RING,)), dma((HEAD,)), dma((3,)), dma((3,)),
            dma((NU, 3)), dma((NU, 3)), dma((NU, 3)), dma((NU, 3)), dma((NU,)),
            dma((NU, NQ)), dma((NU, NQ)), dma((2,)), dma((2, WSLOT)),
        ],
        compiler_params=pltpu.CompilerParams(dimension_semantics=("arbitrary",), vmem_limit_bytes=67043328, collective_id=0, has_side_effects=True),
        cost_estimate=pl.CostEstimate(flops=6 * tokens * width * ff, bytes_accessed=4 * SUB * NU * width * ff, transcendentals=tokens * ff),
        name="steps",
    )(lens, pnt, pn_pair, x2, ws_in, ws_out, w_in, w_out)


def combine_kernel(tok, c_ref, y2_ref, ys_ref, out_ref):
    n_arr = ys_ref.shape[0]
    for p in range(ys_ref.shape[2] // (2 * SUB)):
        ys = jnp.concatenate([ys_ref[a, 0, p * 2 * SUB:(p + 1) * 2 * SUB, :] for a in range(n_arr)], axis=0)
        r = slice(p * 2 * tok, (p + 1) * 2 * tok)
        y1 = jnp.dot(c_ref[r, :], ys, preferred_element_type=F32)
        out_ref[r, :] = (y1 + y2_ref[r, :]).astype(BF16)


def combine_call(c, y2, ys, tok):
    tokens, width = y2.shape
    n_arr, steps, rows, _ = ys.shape
    tile = tokens // steps
    return pl.pallas_call(
        functools.partial(combine_kernel, tok),
        grid=(steps,),
        in_specs=[
            pl.BlockSpec((tile, c.shape[1]), lambda i: (i, 0)),
            pl.BlockSpec((tile, width), lambda i: (i, 0)),
            pl.BlockSpec((n_arr, 1, rows, width), lambda i: (0, i, 0, 0)),
        ],
        out_specs=pl.BlockSpec((tile, width), lambda i: (i, 0)),
        out_shape=jax.ShapeDtypeStruct((tokens, width), BF16),
        compiler_params=params(("arbitrary",), 60),
        cost_estimate=pl.CostEstimate(flops=2 * tokens * width * c.shape[1], bytes_accessed=8 * tokens * width, transcendentals=0),
        name="combine",
    )(c, y2, ys)


def solution(mesh):
    tok_spec = P('data', 'seq', None)
    expert_spec = P('seq', None, None)

    def per_device(x_blk, len_blk, phi_slots, scale_g, w_in, w_out, ws_in, ws_out):
        batch, tok, width = x_blk.shape
        d = lax.axis_index('data')
        s = lax.axis_index('seq')
        cb, xb = s % 2, s // 2
        pn = (scale_g * unit_rows(phi_slots, 0)).astype(BF16)
        pr = pn.reshape(width, 2, 2, 2, NU, SUB)
        for axis, bit in ((1, xb), (2, cb), (3, d)):
            pr = jnp.where(bit == 1, jnp.flip(pr, axis), pr)
        pr = pr.transpose(0, 2, 4, 1, 3, 5)
        pnt = pr.reshape(width, -1).T
        pn_pair = jnp.broadcast_to(pr.reshape(width, -1, 1, SUB), (width, 2 * NU * NQ, 2, SUB)).reshape(width, -1)

        x2 = x_blk.reshape(batch * tok, width)
        y2, c, ys = step_call(len_blk, pnt, pn_pair, x2, ws_in, ws_out, w_in, w_out, tok)
        return combine_call(c, y2, ys, tok).reshape(batch, tok, width)

    return jax.shard_map(per_device, mesh=mesh, in_specs=(tok_spec, P('data'), P(), P(), expert_spec, expert_spec, P(), P()), out_specs=tok_spec, check_vma=False)
```

```python
import functools
import math

import jax
import jax.numpy as jnp
from jax import lax
from jax.experimental import pallas as pl
from jax.experimental.pallas import tpu as pltpu
from jax.sharding import PartitionSpec as P

NORM_EPS = 1e-6
NEG_BIG = -1e30
F32 = jnp.float32
BF16 = jnp.bfloat16
GELU_A = (2.0 / math.pi) ** 0.5
GELU_B = 0.044715 * GELU_A
SUB = 8
NU = 2
NQ = 4


def unit_rows(values, axis_id):
    wide_vals = values.astype(F32)
    return wide_vals / jnp.sqrt(jnp.sum(wide_vals * wide_vals, axis=axis_id, keepdims=True) + NORM_EPS)


def row_unit(x):
    xf = x.astype(F32)
    return (xf * lax.rsqrt(jnp.sum(xf * xf, axis=-1, keepdims=True) + NORM_EPS)).astype(BF16)


def params(sem, vmem_mb):
    return pltpu.CompilerParams(dimension_semantics=sem, vmem_limit_bytes=vmem_mb << 20)


def gelu(h):
    return h * (0.5 + 0.5 * jnp.tanh(h * (GELU_A + GELU_B * (h * h))))


HEAD = 16
D_A, D_B, D_C = 3, 1, 12
T_E0 = HEAD + D_A
T_DB = T_E0 + SUB
T_E1 = T_DB + D_B
T_DC = T_E1 + SUB
STEPS = T_DC + D_C
T_FWD = (T_DC + 3, T_DC + 10)
LAG = 3
GRP = 2
NGRP = HEAD // GRP
RING = 4
WSLOT = 3


def pick(t, head, e0, e1):
    late = jnp.where(t < T_E1, t - HEAD - SUB, jnp.where(t < T_DC, e1, t - HEAD - 2 * SUB))
    early = jnp.where(t < T_E0, t - HEAD, jnp.where(t < T_DB, e0, late))
    return jnp.where(t < HEAD, head, early)


def x_tile(t):
    return pick(t, t, D_A, D_A + D_B)


def out_tile(t):
    return pick(t, 0, D_A - 1, D_A + D_B - 1)


def ys_index(rc, u, q):
    return (rc * NU + u) * NQ + q


def step_kernel(
    tok, len_ref, pnt_ref, pn_ref, x_ref, ws1_hbm, ws2_hbm, w1_hbm, w2_hbm,
    y2_ref, c_ref, ys_ref,
    ring, keep, recv, drecv, st, st_in, w1, w2, ew1, ew2, s_a, s_b, xs,
    ring_send, p_recv, st_send, st_recv, d_send, d_recv, r_send, r_recv, own_sem, f_send, f_recv, w_sem, e_sem,
):
    t = pl.program_id(0)
    d = lax.axis_index('data')
    s = lax.axis_index('seq')
    core = s + 1 - 2 * (s % 2)
    owned = w1_hbm.shape[0] // 2
    ff = w1.shape[1]
    half_ff = ff // 2
    nb = x_ref.shape[0] // tok
    slots = pnt_ref.shape[0]
    batch = HEAD * nb
    rows = nb * SUB
    lanes = s_a.shape[0]

    def peer(rx, rh):
        return (d + rh * (1 - 2 * d), (s + 2 * rx) % 4)

    def remote(src, dst, send, rec, dev):
        return pltpu.make_async_remote_copy(src_ref=src, dst_ref=dst, send_sem=send, recv_sem=rec, device_id=dev, device_id_type=pl.DeviceIdType.MESH)

    def p_copy(i):
        return remote(ring.at[i % RING], recv.at[i], ring_send.at[i % RING], p_recv.at[i], (d, core))

    def st_copy(k, i):
        return remote(st.at[i], st_in.at[k, i], st_send.at[k, i], st_recv.at[k, i], (d, (core, (s + 2) % 4, 3 - s)[k]))

    def d_copy(u, q, g):
        p = pl.ds(0, HEAD) if u else pl.ds(g * GRP, GRP)
        return remote(keep.at[p, u, q], drecv.at[u, q - 1, p], d_send.at[u, q - 1, g], d_recv.at[u, q - 1, g], peer(q // 2, q % 2))

    def d_copies(u):
        return [d_copy(u, q, g) for g in range(1 if u else NGRP) for q in (3, 2, 1)]

    def r_copy(u, q):
        return remote(recv.at[:, u, q % 2], ys_ref.at[ys_index(0, u, q)], r_send.at[u, q - 1], r_recv.at[u, q - 1], peer(q // 2, q % 2))

    def own_copy(u):
        return pltpu.make_async_copy(recv.at[:, u, 0], ys_ref.at[ys_index(0, u, 0)], own_sem.at[u])

    def f_copy(u, q):
        src = recv.at[:, u, 0] if q == 0 else ys_ref.at[ys_index(0, u, q)]
        return remote(src, ys_ref.at[ys_index(1, u, q)], f_send.at[u, q], f_recv.at[u, q], (d, core))

    def w_copies():
        return (pltpu.make_async_copy(ws1_hbm, w1, w_sem.at[0]), pltpu.make_async_copy(ws2_hbm, w2, w_sem.at[1]))

    def e_copies(n):
        e = d * owned + n // 2
        cols = pl.ds(pl.multiple_of((n % 2) * half_ff, 128), half_ff)
        k = n % WSLOT
        return (
            pltpu.make_async_copy(w1_hbm.at[e, :, cols], ew1.at[k], e_sem.at[0, k]),
            pltpu.make_async_copy(w2_hbm.at[e, cols, :], ew2.at[k], e_sem.at[1, k]),
        )

    @pl.when(t == 0)
    def _():
        barrier = pltpu.get_barrier_semaphore()
        for dev in ((d, core), (d, (s + 2) % 4), (d, 3 - s), peer(0, 1), peer(1, 1)):
            pl.semaphore_signal(barrier, inc=1, device_id=dev, device_id_type=pl.DeviceIdType.MESH)
        pl.semaphore_wait(barrier, 5)

    @pl.when(t == 1)
    def _():
        for cp in w_copies():
            cp.start()

    @pl.when((t > 0) & (t <= HEAD))
    def _():
        p_copy(t - 1).start()
        for k in range(3):
            st_copy(k, t - 1).start()

    @pl.when((t >= LAG + GRP) & (t <= HEAD + 1) & ((t - LAG) % GRP == 0))
    def _():
        for q in (3, 2, 1):
            d_copy(0, q, (t - LAG) // GRP - 1).start()

    @pl.when(t == HEAD + 2)
    def _():
        for q in (3, 2, 1):
            d_copy(0, q, NGRP - 1).start()
        for q in (3, 2, 1):
            d_copy(1, q, 0).start()

    @pl.when(t < HEAD)
    def _():
        @pl.when(t >= RING)
        def _():
            p_copy(t - RING).wait_send()

        lane = lax.broadcasted_iota(jnp.int32, (slots, tok), 1)
        base = s * tok
        cols = jnp.zeros((slots, slots), F32)
        col = lax.broadcasted_iota(jnp.int32, cols.shape, 1)
        x = x_ref[...]
        lts = lax.dot_general(pnt_ref[...], row_unit(x), (((1,), (1,)), ((), ())), preferred_element_type=F32)
        es = []
        for i in range(nb):
            b = t * nb + i
            lt = lts[:, i * tok:(i + 1) * tok]
            valid = (base + lane) < len_ref[b]
            m = jnp.max(jnp.where(valid, lt, NEG_BIG), axis=1, keepdims=True)
            e = jnp.where(valid, jnp.exp(lt - m), 0.0)
            z = jnp.sum(e, axis=1, keepdims=True)
            cols = jnp.where(col == i, m, jnp.where(col == nb + i, z, cols))
            es.append(e.astype(BF16))
        nums = [jnp.dot(es[i], x[i * tok:(i + 1) * tok], preferred_element_type=F32) for i in range(nb)]
        for i in range(0, nb, 2):
            for u in range(NU):
                for q in range(NQ):
                    for rc in range(2):
                        r = ys_index(rc, u, q) * SUB
                        pair = jnp.concatenate([nums[i][r:r + SUB], nums[i + 1][r:r + SUB]], axis=0).astype(BF16)
                        if rc == 0:
                            keep[t, u, q, i * SUB:(i + 2) * SUB, :] = pair
                        else:
                            ring[t % RING, u, q, i * SUB:(i + 2) * SUB, :] = pair
        st[t] = cols.T[:2 * nb]

    @pl.when(t == HEAD)
    def _():
        for n in range(WSLOT):
            for cp in e_copies(n):
                cp.start()
        for cp in w_copies():
            cp.wait()
        for i in range(HEAD - RING, HEAD):
            p_copy(i).wait_send()

    def merge(i):
        p_copy(i).wait_recv()
        for k in range(3):
            st_copy(k, i).wait()
        lane = lax.broadcasted_iota(jnp.int32, (2 * nb, slots), 1)
        hop = slots // 8

        def over_x(v):
            return jnp.where((lane // hop) % 2 == 0, pltpu.roll(v, slots - hop, 1), pltpu.roll(v, hop, 1))

        peers = (st[i], pltpu.roll(st_in[0, i], slots // 2, 1), over_x(st_in[1, i]), over_x(pltpu.roll(st_in[2, i], slots // 2, 1)))
        ms = [v[:nb] for v in peers]
        zs = [v[nb:] for v in peers]
        top = jnp.maximum(jnp.maximum(ms[0], ms[1]), jnp.maximum(ms[2], ms[3]))
        ws = [jnp.exp(m - top) for m in ms]
        inv = 1.0 / (ws[0] * zs[0] + ws[1] * zs[1] + ws[2] * zs[2] + ws[3] * zs[3])
        both = jnp.concatenate([ws[0] * inv, ws[1] * inv], axis=0)
        w = jnp.concatenate([both] * (slots // (2 * nb)), axis=0).T
        for u in range(NU):
            for q in range(NQ):
                row = slice(ys_index(0, u, q) * SUB, ys_index(0, u, q) * SUB + SUB)
                for j in range(0, nb, 2):
                    r = slice(j * SUB, (j + 2) * SUB)
                    kk = keep[i, u, q, r, :].astype(F32)
                    rr = recv[i, u, q, r, :].astype(F32)
                    out = []
                    for o in range(2):
                        ro = slice(o * SUB, (o + 1) * SUB)
                        c0 = j + o
                        out.append(kk[ro] * w[row, c0:c0 + 1] + rr[ro] * w[row, nb + c0:nb + c0 + 1])
                    keep[i, u, q, r, :] = jnp.concatenate(out, axis=0).astype(BF16)

    @pl.when((t >= LAG) & (t <= HEAD))
    def _():
        merge(t - LAG)

    @pl.when(t == HEAD + 1)
    def _():
        @pl.loop(HEAD + 1 - LAG, HEAD)
        def _(i):
            merge(i)

    def unpack(u):
        for cp in d_copies(u):
            cp.wait_recv()

        @pl.loop(0, HEAD)
        def _(i):
            r = pl.ds(pl.multiple_of(i * rows, rows), rows)
            a = keep[i, u, 0].astype(F32) + drecv[u, 1, i].astype(F32)
            b = drecv[u, 0, i].astype(F32) + drecv[u, 2, i].astype(F32)
            for k in range(lanes):
                s_a[k, r, :] = a[:, k * 128:(k + 1) * 128]
                s_b[k, r, :] = b[:, k * 128:(k + 1) * 128]

    def pack(u):
        @pl.loop(0, HEAD)
        def _(i):
            r = pl.ds(pl.multiple_of(i * rows, rows), rows)
            for k in range(lanes):
                cols = slice(k * 128, (k + 1) * 128)
                recv[i, u, 0, :, cols] = s_a[k, r, :].astype(BF16)
                recv[i, u, 1, :, cols] = s_b[k, r, :].astype(BF16)

    @pl.when(t == T_E0)
    def _():
        unpack(0)

    @pl.when(t == T_E1)
    def _():
        unpack(1)

    is_e = ((t >= T_E0) & (t < T_DB)) | ((t >= T_E1) & (t < T_DC))

    @pl.when(is_e)
    def _():
        k_all = jnp.where(t < T_DB, t - T_E0, t - T_E1 + SUB)
        e = k_all % SUB
        for k in range(lanes):
            cols = slice(k * 128, (k + 1) * 128)
            xs[:batch, cols] = s_a[k, pl.ds(e, batch, stride=SUB), :].astype(BF16)
            xs[batch:, cols] = s_b[k, pl.ds(e, batch, stride=SUB), :].astype(BF16)

        def half(n):
            for cp in e_copies(n):
                cp.wait()
            k = n % WSLOT
            xv = xs[...]
            nc = 3
            fb = half_ff // nc

            def up(j):
                return jnp.dot(xv, ew1[k, :, j * fb:(j + 1) * fb], preferred_element_type=F32)

            y = None
            h = up(0)
            for j in range(nc):
                nxt = up(j + 1) if j + 1 < nc else None
                v = jnp.dot(gelu(h).astype(BF16), ew2[k, j * fb:(j + 1) * fb, :], preferred_element_type=F32)
                y = v if y is None else y + v
                h = nxt

            for k in range(lanes):
                cols = slice(k * 128, (k + 1) * 128)
                pa = pl.ds(e, batch, stride=SUB)

                @pl.when(n % 2 == 0)
                def _(k=k, cols=cols):
                    s_a[k, pa, :] = y[:batch, cols]
                    s_b[k, pa, :] = y[batch:, cols]

                @pl.when(n % 2 == 1)
                def _(k=k, cols=cols):
                    s_a[k, pa, :] += y[:batch, cols]
                    s_b[k, pa, :] += y[batch:, cols]

            @pl.when(n + WSLOT < 2 * owned)
            def _():
                for cp in e_copies(n + WSLOT):
                    cp.start()

        @pl.loop(0, 2)
        def _(hh):
            half(2 * k_all + hh)

    def give(u):
        pack(u)

    @pl.when(t == T_DB - 1)
    def _():
        give(0)

    @pl.when(t == T_DC - 1)
    def _():
        give(1)

    def send_back(u):
        for q in (3, 2, 1):
            r_copy(u, q).start()
        own_copy(u).start()
        f_copy(u, 0).start()

    @pl.when(t == T_DB)
    def _():
        send_back(0)

    @pl.when(t == T_DC)
    def _():
        send_back(1)

    def forward(u):
        for q in (1, 2, 3):
            r_copy(u, q).wait_recv()
            f_copy(u, q).start()

    @pl.when(t == T_FWD[0])
    def _():
        forward(0)

    @pl.when(t == T_FWD[1])
    def _():
        forward(1)

    @pl.when((t >= HEAD) & jnp.logical_not(is_e))
    def _():
        xn = row_unit(x_ref[...])
        logits = jnp.dot(xn, pn_ref[...], preferred_element_type=F32)
        ti = lax.broadcasted_iota(jnp.int32, logits.shape, 0)
        si = lax.broadcasted_iota(jnp.int32, logits.shape, 1)
        mine = ((ti // tok) % 2) == ((si // SUB) % 2)
        logits = jnp.where(mine, logits, NEG_BIG)
        ex = jnp.exp(logits - jnp.max(logits, axis=1, keepdims=True))
        c_ref[...] = (ex / jnp.sum(ex, axis=1, keepdims=True)).astype(BF16)
        nf = 3
        fb = ff // nf

        def up(j):
            return jnp.dot(xn, w1[:, j * fb:(j + 1) * fb], preferred_element_type=F32)

        h = up(0)
        for j in range(nf):
            nxt = up(j + 1) if j + 1 < nf else None
            y = jnp.dot(gelu(h).astype(BF16), w2[j * fb:(j + 1) * fb, :], preferred_element_type=F32)
            if j == 0:
                y2_ref[...] = y
            else:
                y2_ref[...] += y
            h = nxt

    @pl.when(t == STEPS - 1)
    def _():
        for u in range(NU):
            own_copy(u).wait()
            for cp in d_copies(u):
                cp.wait_send()
            for q in (1, 2, 3):
                r_copy(u, q).wait_send()
            for q in range(NQ):
                f_copy(u, q).wait()


def step_call(lens, pnt, pn_pair, x2, ws_in, ws_out, w_in, w_out, tok):
    tokens, width = x2.shape
    ff = ws_in.shape[1]
    cols = pn_pair.shape[1]
    slots = pnt.shape[0]
    tile = tokens // HEAD
    nb = tile // tok
    rows = nb * SUB
    batch = HEAD * nb
    hbm = pl.BlockSpec(memory_space=pl.ANY)
    dma = pltpu.SemaphoreType.DMA
    return pl.pallas_call(
        functools.partial(step_kernel, tok),
        grid=(STEPS,),
        in_specs=[
            pl.BlockSpec(memory_space=pltpu.SMEM),
            pl.BlockSpec((slots, width), lambda t: (0, 0)),
            pl.BlockSpec((width, cols), lambda t: (0, 0)),
            pl.BlockSpec((tile, width), lambda t: (x_tile(t), 0)),
            hbm, hbm, hbm, hbm,
        ],
        out_specs=[
            pl.BlockSpec((tile, width), lambda t: (out_tile(t), 0)),
            pl.BlockSpec((tile, cols), lambda t: (out_tile(t), 0)),
            hbm,
        ],
        out_shape=[
            jax.ShapeDtypeStruct((tokens, width), F32),
            jax.ShapeDtypeStruct((tokens, cols), BF16),
            jax.ShapeDtypeStruct((2 * NU * NQ, HEAD, rows, width), BF16),
        ],
        scratch_shapes=[
            pltpu.VMEM((RING, NU, NQ, rows, width), BF16),
            pltpu.VMEM((HEAD, NU, NQ, rows, width), BF16),
            pltpu.VMEM((HEAD, NU, NQ, rows, width), BF16),
            pltpu.VMEM((NU, 3, HEAD, rows, width), BF16),
            pltpu.VMEM((HEAD, 2 * nb, slots), F32),
            pltpu.VMEM((3, HEAD, 2 * nb, slots), F32),
            pltpu.VMEM((width, ff), BF16),
            pltpu.VMEM((ff, width), BF16),
            pltpu.VMEM((WSLOT, width, ff // 2), BF16),
            pltpu.VMEM((WSLOT, ff // 2, width), BF16),
            pltpu.VMEM((width // 128, batch * SUB, 128), F32),
            pltpu.VMEM((width // 128, batch * SUB, 128), F32),
            pltpu.VMEM((2 * batch, width), BF16),
            dma((RING,)), dma((HEAD,)), dma((3, HEAD)), dma((3, HEAD)),
            dma((NU, 3, NGRP)), dma((NU, 3, NGRP)), dma((NU, 3)), dma((NU, 3)), dma((NU,)),
            dma((NU, NQ)), dma((NU, NQ)), dma((2,)), dma((2, WSLOT)),
        ],
        compiler_params=pltpu.CompilerParams(dimension_semantics=("arbitrary",), vmem_limit_bytes=67043328, collective_id=0, has_side_effects=True),
        cost_estimate=pl.CostEstimate(flops=6 * tokens * width * ff, bytes_accessed=4 * SUB * NU * width * ff, transcendentals=tokens * ff),
        name="steps",
    )(lens, pnt, pn_pair, x2, ws_in, ws_out, w_in, w_out)


def combine_kernel(tok, c_ref, y2_ref, ys_ref, out_ref):
    n_arr = ys_ref.shape[0]
    for p in range(ys_ref.shape[2] // (2 * SUB)):
        ys = jnp.concatenate([ys_ref[a, 0, p * 2 * SUB:(p + 1) * 2 * SUB, :] for a in range(n_arr)], axis=0)
        r = slice(p * 2 * tok, (p + 1) * 2 * tok)
        y1 = jnp.dot(c_ref[r, :], ys, preferred_element_type=F32)
        out_ref[r, :] = (y1 + y2_ref[r, :]).astype(BF16)


def combine_call(c, y2, ys, tok):
    tokens, width = y2.shape
    n_arr, steps, rows, _ = ys.shape
    tile = tokens // steps
    return pl.pallas_call(
        functools.partial(combine_kernel, tok),
        grid=(steps,),
        in_specs=[
            pl.BlockSpec((tile, c.shape[1]), lambda i: (i, 0)),
            pl.BlockSpec((tile, width), lambda i: (i, 0)),
            pl.BlockSpec((n_arr, 1, rows, width), lambda i: (0, i, 0, 0)),
        ],
        out_specs=pl.BlockSpec((tile, width), lambda i: (i, 0)),
        out_shape=jax.ShapeDtypeStruct((tokens, width), BF16),
        compiler_params=params(("arbitrary",), 60),
        cost_estimate=pl.CostEstimate(flops=2 * tokens * width * c.shape[1], bytes_accessed=8 * tokens * width, transcendentals=0),
        name="combine",
    )(c, y2, ys)


def solution(mesh):
    tok_spec = P('data', 'seq', None)
    expert_spec = P('seq', None, None)

    def per_device(x_blk, len_blk, phi_slots, scale_g, w_in, w_out, ws_in, ws_out):
        batch, tok, width = x_blk.shape
        d = lax.axis_index('data')
        s = lax.axis_index('seq')
        cb, xb = s % 2, s // 2
        pn = (scale_g * unit_rows(phi_slots, 0)).astype(BF16)
        pr = pn.reshape(width, 2, 2, 2, NU, SUB)
        for axis, bit in ((1, xb), (2, cb), (3, d)):
            pr = jnp.where(bit == 1, jnp.flip(pr, axis), pr)
        pr = pr.transpose(0, 2, 4, 1, 3, 5)
        pnt = pr.reshape(width, -1).T
        pn_pair = jnp.broadcast_to(pr.reshape(width, -1, 1, SUB), (width, 2 * NU * NQ, 2, SUB)).reshape(width, -1)

        x2 = x_blk.reshape(batch * tok, width)
        y2, c, ys = step_call(len_blk, pnt, pn_pair, x2, ws_in, ws_out, w_in, w_out, tok)
        return combine_call(c, y2, ys, tok).reshape(batch, tok, width)

    return jax.shard_map(per_device, mesh=mesh, in_specs=(tok_spec, P('data'), P(), P(), expert_spec, expert_spec, P(), P()), out_specs=tok_spec, check_vma=False)
```

```python
import functools
import math

import jax
import jax.numpy as jnp
from jax import lax
from jax.experimental import pallas as pl
from jax.experimental.pallas import tpu as pltpu
from jax.sharding import PartitionSpec as P

NORM_EPS = 1e-6
NEG_BIG = -1e30
F32 = jnp.float32
BF16 = jnp.bfloat16
GELU_A = (2.0 / math.pi) ** 0.5
GELU_B = 0.044715 * GELU_A
SUB = 8
NU = 2
NQ = 4


def unit_rows(values, axis_id):
    wide_vals = values.astype(F32)
    return wide_vals / jnp.sqrt(jnp.sum(wide_vals * wide_vals, axis=axis_id, keepdims=True) + NORM_EPS)


def row_unit(x):
    xf = x.astype(F32)
    return (xf * lax.rsqrt(jnp.sum(xf * xf, axis=-1, keepdims=True) + NORM_EPS)).astype(BF16)


def params(sem, vmem_mb):
    return pltpu.CompilerParams(dimension_semantics=sem, vmem_limit_bytes=vmem_mb << 20)


def gelu(h):
    return h * (0.5 + 0.5 * jnp.tanh(h * (GELU_A + GELU_B * (h * h))))


HEAD = 16
D_A, D_B, D_C = 5, 2, 9
T_FWD = (3, 8)
RING = 4
WSLOT = 3


def ys_index(rc, u, q):
    return (rc * NU + u) * NQ + q


def step_kernel(
    tok, len_ref, pnt_ref, pn_ref, x_hbm, ws1_hbm, ws2_hbm, w1_hbm, w2_hbm,
    y2_hbm, c_hbm, ys_ref,
    xbuf, y2buf, cbuf, ring, keep, recv, drecv, st, st_in, w1, w2, ew1, ew2, s_a, s_b, xs,
    x_sem, y2_sem, c_sem,
    ring_send, p_recv, st_send, st_recv, d_send, d_recv, r_send, r_recv, own_sem, f_send, f_recv, w_sem, e_sem,
):
    d = lax.axis_index('data')
    s = lax.axis_index('seq')
    core = s + 1 - 2 * (s % 2)
    owned = w1_hbm.shape[0] // 2
    ff = w1.shape[1]
    half_ff = ff // 2
    tile = xbuf.shape[1]
    nb = tile // tok
    slots = pnt_ref.shape[0]
    batch = HEAD * nb
    rows = nb * SUB
    lanes = s_a.shape[0]

    def peer(rx, rh):
        return (d + rh * (1 - 2 * d), (s + 2 * rx) % 4)

    def remote(src, dst, send, rec, dev):
        return pltpu.make_async_remote_copy(src_ref=src, dst_ref=dst, send_sem=send, recv_sem=rec, device_id=dev, device_id_type=pl.DeviceIdType.MESH)

    def p_copy(i):
        return remote(ring.at[i % RING], recv.at[i], ring_send.at[i % RING], p_recv.at[i], (d, core))

    def st_copy(k):
        return remote(st, st_in.at[k], st_send.at[k], st_recv.at[k], (d, (core, (s + 2) % 4, 3 - s)[k]))

    def d_copy(u, q):
        return remote(keep.at[:, u, q], drecv.at[u, q - 1], d_send.at[u, q - 1], d_recv.at[u, q - 1], peer(q // 2, q % 2))

    def r_copy(u, q):
        return remote(recv.at[:, u, q % 2], ys_ref.at[ys_index(0, u, q)], r_send.at[u, q - 1], r_recv.at[u, q - 1], peer(q // 2, q % 2))

    def own_copy(u):
        return pltpu.make_async_copy(recv.at[:, u, 0], ys_ref.at[ys_index(0, u, 0)], own_sem.at[u])

    def f_copy(u, q):
        src = recv.at[:, u, 0] if q == 0 else ys_ref.at[ys_index(0, u, q)]
        return remote(src, ys_ref.at[ys_index(1, u, q)], f_send.at[u, q], f_recv.at[u, q], (d, core))

    def w_copies():
        return (pltpu.make_async_copy(ws1_hbm, w1, w_sem.at[0]), pltpu.make_async_copy(ws2_hbm, w2, w_sem.at[1]))

    def e_copies(n):
        e = d * owned + n // 2
        cols = pl.ds(pl.multiple_of((n % 2) * half_ff, 128), half_ff)
        k = n % WSLOT
        return (
            pltpu.make_async_copy(w1_hbm.at[e, :, cols], ew1.at[k], e_sem.at[0, k]),
            pltpu.make_async_copy(w2_hbm.at[e, cols, :], ew2.at[k], e_sem.at[1, k]),
        )

    def x_copy(n):
        src = x_hbm.at[pl.ds(pl.multiple_of((n % HEAD) * tile, tile), tile), :]
        return pltpu.make_async_copy(src, xbuf.at[n % 2], x_sem.at[n % 2])

    def out_copies(j):
        r = pl.ds(pl.multiple_of(j * tile, tile), tile)
        k = j % 2
        return (
            pltpu.make_async_copy(y2buf.at[k], y2_hbm.at[r, :], y2_sem.at[k]),
            pltpu.make_async_copy(cbuf.at[k], c_hbm.at[r, :], c_sem.at[k]),
        )

    x_copy(0).start()
    barrier = pltpu.get_barrier_semaphore()
    for dev in ((d, core), (d, (s + 2) % 4), (d, 3 - s), peer(0, 1), peer(1, 1)):
        pl.semaphore_signal(barrier, inc=1, device_id=dev, device_id_type=pl.DeviceIdType.MESH)
    for cp in w_copies():
        cp.start()
    st[...] = jnp.zeros_like(st)
    pl.semaphore_wait(barrier, 5)

    @pl.loop(0, HEAD)
    def _(t):
        x_copy(t).wait()
        x_copy(t + 1).start()

        @pl.when(t > 0)
        def _():
            p_copy(t - 1).start()

        @pl.when(t >= RING)
        def _():
            p_copy(t - RING).wait_send()

        lane = lax.broadcasted_iota(jnp.int32, (slots, tok), 1)
        base = s * tok
        stv = st[...]
        stl = lax.broadcasted_iota(jnp.int32, stv.shape, 1)
        x = xbuf[t % 2]
        lts = lax.dot_general(pnt_ref[...], row_unit(x), (((1,), (1,)), ((), ())), preferred_element_type=F32)
        es = []
        for i in range(nb):
            b = t * nb + i
            lt = lts[:, i * tok:(i + 1) * tok]
            valid = (base + lane) < len_ref[b]
            m = jnp.max(jnp.where(valid, lt, NEG_BIG), axis=1, keepdims=True)
            e = jnp.where(valid, jnp.exp(lt - m), 0.0)
            z = jnp.sum(e, axis=1, keepdims=True)
            stv = jnp.where(stl == b, m, jnp.where(stl == batch + b, z, stv))
            es.append(e.astype(BF16))
        nums = [jnp.dot(es[i], x[i * tok:(i + 1) * tok], preferred_element_type=F32) for i in range(nb)]
        for i in range(0, nb, 2):
            for u in range(NU):
                for q in range(NQ):
                    for rc in range(2):
                        r = ys_index(rc, u, q) * SUB
                        pair = jnp.concatenate([nums[i][r:r + SUB], nums[i + 1][r:r + SUB]], axis=0).astype(BF16)
                        if rc == 0:
                            keep[t, u, q, i * SUB:(i + 2) * SUB, :] = pair
                        else:
                            ring[t % RING, u, q, i * SUB:(i + 2) * SUB, :] = pair
        st[...] = stv

    p_copy(HEAD - 1).start()
    for k in range(3):
        st_copy(k).start()
    for n in range(WSLOT):
        for cp in e_copies(n):
            cp.start()
    for cp in w_copies():
        cp.wait()
    for k in range(3):
        st_copy(k).wait()

    @pl.loop(0, HEAD)
    def _(i):
        p_copy(i).wait_recv()

    for i in range(HEAD - RING, HEAD):
        p_copy(i).wait_send()

    def merge(u):
        @pl.loop(0, NQ)
        def _(n):
            q = NQ - 1 - n
            qx = (q + 2) % 4

            def stat(ref, rc, qq):
                return ref[pl.ds(pl.multiple_of(ys_index(rc, u, qq) * SUB, SUB), SUB), :]

            peers = (stat(st, 0, q), stat(st_in.at[0], 1, q), stat(st_in.at[1], 0, qx), stat(st_in.at[2], 1, qx))
            ms = [r[:, :batch] for r in peers]
            zs = [r[:, batch:] for r in peers]
            top = jnp.maximum(jnp.maximum(ms[0], ms[1]), jnp.maximum(ms[2], ms[3]))
            ws = [jnp.exp(m - top) for m in ms]
            inv = 1.0 / (ws[0] * zs[0] + ws[1] * zs[1] + ws[2] * zs[2] + ws[3] * zs[3])
            wk = ws[0] * inv
            wr = ws[1] * inv
            for i in range(HEAD):
                for j in range(0, nb, 2):
                    r = slice(j * SUB, (j + 2) * SUB)
                    kk = keep[i, u, q, r, :].astype(F32)
                    rr = recv[i, u, q, r, :].astype(F32)
                    both = []
                    for o in range(2):
                        b = i * nb + j + o
                        ro = slice(o * SUB, (o + 1) * SUB)
                        both.append(kk[ro] * wk[:, b:b + 1] + rr[ro] * wr[:, b:b + 1])
                    keep[i, u, q, r, :] = jnp.concatenate(both, axis=0).astype(BF16)

            @pl.when(n > 0)
            def _():
                d_copy(u, q + 1).start()

    merge(0)
    merge(1)

    def unpack(u):
        for q in (1, 2, 3):
            d_copy(u, q).wait_recv()

        @pl.loop(0, HEAD)
        def _(i):
            r = pl.ds(pl.multiple_of(i * rows, rows), rows)
            a = keep[i, u, 0].astype(F32) + drecv[u, 1, i].astype(F32)
            b = drecv[u, 0, i].astype(F32) + drecv[u, 2, i].astype(F32)
            for k in range(lanes):
                s_a[k, r, :] = a[:, k * 128:(k + 1) * 128]
                s_b[k, r, :] = b[:, k * 128:(k + 1) * 128]

    def pack(u):
        @pl.loop(0, HEAD)
        def _(i):
            r = pl.ds(pl.multiple_of(i * rows, rows), rows)
            for k in range(lanes):
                cols = slice(k * 128, (k + 1) * 128)
                recv[i, u, 0, :, cols] = s_a[k, r, :].astype(BF16)
                recv[i, u, 1, :, cols] = s_b[k, r, :].astype(BF16)

    def experts(u):
        unpack(u)

        @pl.loop(0, SUB)
        def _(e):
            pa = pl.ds(e, batch, stride=SUB)
            for k in range(lanes):
                cols = slice(k * 128, (k + 1) * 128)
                xs[:batch, cols] = s_a[k, pa, :].astype(BF16)
                xs[batch:, cols] = s_b[k, pa, :].astype(BF16)
            nc = 3
            fb = half_ff // nc
            xv = xs[...]

            def half(n):
                for cp in e_copies(n):
                    cp.wait()
                w = n % WSLOT

                def up(j):
                    return jnp.dot(xv, ew1[w, :, j * fb:(j + 1) * fb], preferred_element_type=F32)

                y = None
                h = up(0)
                for j in range(nc):
                    nxt = up(j + 1) if j + 1 < nc else None
                    v = jnp.dot(gelu(h).astype(BF16), ew2[w, j * fb:(j + 1) * fb, :], preferred_element_type=F32)
                    y = v if y is None else y + v
                    h = nxt

                @pl.when(n + WSLOT < 2 * owned)
                def _():
                    for cp in e_copies(n + WSLOT):
                        cp.start()

                return y

            n0 = 2 * (u * SUB + e)
            y = half(n0)
            for k in range(lanes):
                cols = slice(k * 128, (k + 1) * 128)
                s_a[k, pa, :] = y[:batch, cols]
                s_b[k, pa, :] = y[batch:, cols]
            y = half(n0 + 1)
            for k in range(lanes):
                cols = slice(k * 128, (k + 1) * 128)
                s_a[k, pa, :] += y[:batch, cols]
                s_b[k, pa, :] += y[batch:, cols]

        pack(u)

    def send_back(u):
        for q in (3, 2, 1):
            r_copy(u, q).start()
        own_copy(u).start()
        f_copy(u, 0).start()

    def forward(u):
        for q in (1, 2, 3):
            r_copy(u, q).wait_recv()
            f_copy(u, q).start()

    def dense(j):
        n = HEAD + j
        k = j % 2
        x_copy(n).wait()

        @pl.when(j + 1 < HEAD)
        def _():
            x_copy(n + 1).start()

        @pl.when(j >= 2)
        def _():
            for cp in out_copies(j - 2):
                cp.wait()

        xn = row_unit(xbuf[n % 2])
        logits = jnp.dot(xn, pn_ref[...], preferred_element_type=F32)
        ti = lax.broadcasted_iota(jnp.int32, logits.shape, 0)
        si = lax.broadcasted_iota(jnp.int32, logits.shape, 1)
        mine = ((ti // tok) % 2) == ((si // SUB) % 2)
        logits = jnp.where(mine, logits, NEG_BIG)
        ex = jnp.exp(logits - jnp.max(logits, axis=1, keepdims=True))
        cbuf[k] = (ex / jnp.sum(ex, axis=1, keepdims=True)).astype(BF16)
        nf = 3
        fb = ff // nf

        def up(f):
            return jnp.dot(xn, w1[:, f * fb:(f + 1) * fb], preferred_element_type=F32)

        h = up(0)
        for f in range(nf):
            nxt = up(f + 1) if f + 1 < nf else None
            y = jnp.dot(gelu(h).astype(BF16), w2[f * fb:(f + 1) * fb, :], preferred_element_type=F32)
            if f == 0:
                y2buf[k] = y
            else:
                y2buf[k] += y
            h = nxt
        for cp in out_copies(j):
            cp.start()

    for u in range(NU):
        @pl.loop(0, (D_A, D_B)[u])
        def _(j, u=u):
            dense(j + (0, D_A)[u])

        experts(u)
        send_back(u)

    @pl.loop(0, D_C)
    def _(j):
        for u in range(NU):

            @pl.when(j == T_FWD[u])
            def _(u=u):
                forward(u)

        dense(j + D_A + D_B)

    for j in (HEAD - 2, HEAD - 1):
        for cp in out_copies(j):
            cp.wait()
    for u in range(NU):
        own_copy(u).wait()
        for q in (1, 2, 3):
            d_copy(u, q).wait_send()
            r_copy(u, q).wait_send()
        for q in range(NQ):
            f_copy(u, q).wait()


def step_call(lens, pnt, pn_pair, x2, ws_in, ws_out, w_in, w_out, tok):
    tokens, width = x2.shape
    ff = ws_in.shape[1]
    cols = pn_pair.shape[1]
    slots = pnt.shape[0]
    tile = tokens // HEAD
    nb = tile // tok
    rows = nb * SUB
    batch = HEAD * nb
    hbm = pl.BlockSpec(memory_space=pl.ANY)
    dma = pltpu.SemaphoreType.DMA
    return pl.pallas_call(
        functools.partial(step_kernel, tok),
        in_specs=[
            pl.BlockSpec(memory_space=pltpu.SMEM),
            pl.BlockSpec(memory_space=pltpu.VMEM),
            pl.BlockSpec(memory_space=pltpu.VMEM),
            hbm, hbm, hbm, hbm, hbm,
        ],
        out_specs=[hbm, hbm, hbm],
        out_shape=[
            jax.ShapeDtypeStruct((tokens, width), F32),
            jax.ShapeDtypeStruct((tokens, cols), BF16),
            jax.ShapeDtypeStruct((2 * NU * NQ, HEAD, rows, width), BF16),
        ],
        scratch_shapes=[
            pltpu.VMEM((2, tile, width), BF16),
            pltpu.VMEM((2, tile, width), F32),
            pltpu.VMEM((2, tile, cols), BF16),
            pltpu.VMEM((RING, NU, NQ, rows, width), BF16),
            pltpu.VMEM((HEAD, NU, NQ, rows, width), BF16),
            pltpu.VMEM((HEAD, NU, NQ, rows, width), BF16),
            pltpu.VMEM((NU, 3, HEAD, rows, width), BF16),
            pltpu.VMEM((slots, 2 * batch), F32),
            pltpu.VMEM((3, slots, 2 * batch), F32),
            pltpu.VMEM((width, ff), BF16),
            pltpu.VMEM((ff, width), BF16),
            pltpu.VMEM((WSLOT, width, ff // 2), BF16),
            pltpu.VMEM((WSLOT, ff // 2, width), BF16),
            pltpu.VMEM((width // 128, batch * SUB, 128), F32),
            pltpu.VMEM((width // 128, batch * SUB, 128), F32),
            pltpu.VMEM((2 * batch, width), BF16),
            dma((2,)), dma((2,)), dma((2,)),
            dma((RING,)), dma((HEAD,)), dma((3,)), dma((3,)),
            dma((NU, 3)), dma((NU, 3)), dma((NU, 3)), dma((NU, 3)), dma((NU,)),
            dma((NU, NQ)), dma((NU, NQ)), dma((2,)), dma((2, WSLOT)),
        ],
        compiler_params=pltpu.CompilerParams(vmem_limit_bytes=67043328, collective_id=0, has_side_effects=True),
        cost_estimate=pl.CostEstimate(flops=6 * tokens * width * ff, bytes_accessed=4 * SUB * NU * width * ff, transcendentals=tokens * ff),
        name="steps",
    )(lens, pnt, pn_pair, x2, ws_in, ws_out, w_in, w_out)


def combine_kernel(tok, c_ref, y2_ref, ys_ref, out_ref):
    n_arr, blocks, rows, _ = ys_ref.shape
    pairs = rows // (2 * SUB)
    for p in range(blocks * pairs):
        lo = (p % pairs) * 2 * SUB
        ys = jnp.concatenate([ys_ref[a, p // pairs, lo:lo + 2 * SUB, :] for a in range(n_arr)], axis=0)
        r = slice(p * 2 * tok, (p + 1) * 2 * tok)
        y1 = jnp.dot(c_ref[r, :], ys, preferred_element_type=F32)
        out_ref[r, :] = (y1 + y2_ref[r, :]).astype(BF16)


def combine_call(c, y2, ys, tok):
    tokens, width = y2.shape
    n_arr, steps, rows, _ = ys.shape
    blocks = 2
    steps //= blocks
    tile = tokens // steps
    return pl.pallas_call(
        functools.partial(combine_kernel, tok),
        grid=(steps,),
        in_specs=[
            pl.BlockSpec((tile, c.shape[1]), lambda i: (i, 0)),
            pl.BlockSpec((tile, width), lambda i: (i, 0)),
            pl.BlockSpec((n_arr, blocks, rows, width), lambda i: (0, i, 0, 0)),
        ],
        out_specs=pl.BlockSpec((tile, width), lambda i: (i, 0)),
        out_shape=jax.ShapeDtypeStruct((tokens, width), BF16),
        compiler_params=params(("arbitrary",), 60),
        cost_estimate=pl.CostEstimate(flops=2 * tokens * width * c.shape[1], bytes_accessed=8 * tokens * width, transcendentals=0),
        name="combine",
    )(c, y2, ys)


def solution(mesh):
    tok_spec = P('data', 'seq', None)
    expert_spec = P('seq', None, None)

    def per_device(x_blk, len_blk, phi_slots, scale_g, w_in, w_out, ws_in, ws_out):
        batch, tok, width = x_blk.shape
        d = lax.axis_index('data')
        s = lax.axis_index('seq')
        cb, xb = s % 2, s // 2
        pn = (scale_g * unit_rows(phi_slots, 0)).astype(BF16)
        pr = pn.reshape(width, 2, 2, 2, NU, SUB)
        for axis, bit in ((1, xb), (2, cb), (3, d)):
            pr = jnp.where(bit == 1, jnp.flip(pr, axis), pr)
        pr = pr.transpose(0, 2, 4, 1, 3, 5)
        pnt = pr.reshape(width, -1).T
        pn_pair = jnp.broadcast_to(pr.reshape(width, -1, 1, SUB), (width, 2 * NU * NQ, 2, SUB)).reshape(width, -1)

        x2 = x_blk.reshape(batch * tok, width)
        y2, c, ys = step_call(len_blk, pnt, pn_pair, x2, ws_in, ws_out, w_in, w_out, tok)
        return combine_call(c, y2, ys, tok).reshape(batch, tok, width)

    return jax.shard_map(per_device, mesh=mesh, in_specs=(tok_spec, P('data'), P(), P(), expert_spec, expert_spec, P(), P()), out_specs=tok_spec, check_vma=False)
```

```python
import functools
import math

import jax
import jax.numpy as jnp
from jax import lax
from jax.experimental import pallas as pl
from jax.experimental.pallas import tpu as pltpu
from jax.sharding import PartitionSpec as P

NORM_EPS = 1e-6
NEG_BIG = -1e30
F32 = jnp.float32
BF16 = jnp.bfloat16
GELU_A = (2.0 / math.pi) ** 0.5
GELU_B = 0.044715 * GELU_A
SUB = 8
NU = 2
NQ = 4


def row_unit(x):
    xf = x.astype(F32)
    return (xf * lax.rsqrt(jnp.sum(xf * xf, axis=-1, keepdims=True) + NORM_EPS)).astype(BF16)


def params(sem, vmem_mb):
    return pltpu.CompilerParams(dimension_semantics=sem, vmem_limit_bytes=vmem_mb << 20)


def gelu(h):
    return h * (0.5 + 0.5 * jnp.tanh(h * (GELU_A + GELU_B * (h * h))))


HEAD = 16
D_A, D_B, D_C = 6, 2, 8
T_FWD = (2, 7)
RING = 4
WSLOT = 3


def ys_index(rc, u, q):
    return (rc * NU + u) * NQ + q


def step_kernel(
    tok, len_ref, g_ref, phi_ref, x_hbm, ws1_hbm, ws2_hbm, w1_hbm, w2_hbm,
    y2_hbm, c_hbm, ys_ref,
    pnf, pnt_ref, pn_ref, xbuf, y2buf, cbuf, ring, keep, recv, drecv, st, st_in, w1, w2, ew1, ew2, s_a, s_b, xs,
    x_sem, y2_sem, c_sem,
    ring_send, p_recv, st_send, st_recv, d_send, d_recv, r_send, r_recv, own_sem, f_send, f_recv, w_sem, e_sem,
):
    d = lax.axis_index('data')
    s = lax.axis_index('seq')
    core = s + 1 - 2 * (s % 2)
    owned = w1_hbm.shape[0] // 2
    ff = w1.shape[1]
    half_ff = ff // 2
    tile = xbuf.shape[1]
    nb = tile // tok
    slots = phi_ref.shape[1]
    batch = HEAD * nb
    rows = nb * SUB
    lanes = s_a.shape[0]

    def peer(rx, rh):
        return (d + rh * (1 - 2 * d), (s + 2 * rx) % 4)

    def remote(src, dst, send, rec, dev):
        return pltpu.make_async_remote_copy(src_ref=src, dst_ref=dst, send_sem=send, recv_sem=rec, device_id=dev, device_id_type=pl.DeviceIdType.MESH)

    def p_copy(i):
        return remote(ring.at[i % RING], recv.at[i], ring_send.at[i % RING], p_recv.at[i], (d, core))

    def st_copy(k):
        return remote(st, st_in.at[k], st_send.at[k], st_recv.at[k], (d, (core, (s + 2) % 4, 3 - s)[k]))

    def d_copy(u, q):
        return remote(keep.at[:, u, q], drecv.at[u, q - 1], d_send.at[u, q - 1], d_recv.at[u, q - 1], peer(q // 2, q % 2))

    def r_copy(u, q):
        return remote(recv.at[:, u, q % 2], ys_ref.at[ys_index(0, u, q)], r_send.at[u, q - 1], r_recv.at[u, q - 1], peer(q // 2, q % 2))

    def own_copy(u):
        return pltpu.make_async_copy(recv.at[:, u, 0], ys_ref.at[ys_index(0, u, 0)], own_sem.at[u])

    def f_copy(u, q):
        src = recv.at[:, u, 0] if q == 0 else ys_ref.at[ys_index(0, u, q)]
        return remote(src, ys_ref.at[ys_index(1, u, q)], f_send.at[u, q], f_recv.at[u, q], (d, core))

    def w_copies():
        return (pltpu.make_async_copy(ws1_hbm, w1, w_sem.at[0]), pltpu.make_async_copy(ws2_hbm, w2, w_sem.at[1]))

    def e_copies(n):
        e = d * owned + n // 2
        cols = pl.ds(pl.multiple_of((n % 2) * half_ff, 128), half_ff)
        k = n % WSLOT
        return (
            pltpu.make_async_copy(w1_hbm.at[e, :, cols], ew1.at[k], e_sem.at[0, k]),
            pltpu.make_async_copy(w2_hbm.at[e, cols, :], ew2.at[k], e_sem.at[1, k]),
        )

    def x_copy(n):
        src = x_hbm.at[pl.ds(pl.multiple_of((n % HEAD) * tile, tile), tile), :]
        return pltpu.make_async_copy(src, xbuf.at[n % 2], x_sem.at[n % 2])

    def out_copies(j):
        r = pl.ds(pl.multiple_of(j * tile, tile), tile)
        k = j % 2
        return (
            pltpu.make_async_copy(y2buf.at[k], y2_hbm.at[r, :], y2_sem.at[k]),
            pltpu.make_async_copy(cbuf.at[k], c_hbm.at[r, :], c_sem.at[k]),
        )

    x_copy(0).start()
    barrier = pltpu.get_barrier_semaphore()
    for dev in ((d, core), (d, (s + 2) % 4), (d, 3 - s), peer(0, 1), peer(1, 1)):
        pl.semaphore_signal(barrier, inc=1, device_id=dev, device_id_type=pl.DeviceIdType.MESH)
    for cp in w_copies():
        cp.start()
    st[...] = jnp.zeros_like(st)
    phi = phi_ref[...].astype(F32)
    inv = g_ref[0] / jnp.sqrt(jnp.sum(phi * phi, axis=0, keepdims=True) + NORM_EPS)
    width = phi.shape[0]
    for k in range(0, width, 128):
        pnf[:, k:k + 128] = (phi[k:k + 128] * inv).T
    for rc in range(2):
        for u in range(NU):
            for q in range(0, NQ):
                sx, sc, sh = (s // 2 + q // 2) % 2, (s + rc) % 2, (d + q) % 2
                src = pl.multiple_of((((sx * 2 + sc) * 2 + sh) * NU + u) * SUB, SUB)
                v = pnf[pl.ds(src, SUB), :]
                r = ys_index(rc, u, q) * SUB
                pn_ref[2 * r:2 * r + 2 * SUB, :] = jnp.concatenate([v, v], axis=0).astype(BF16)
    for r in range(0, slots, 2 * SUB):
        lo = pn_ref[2 * r:2 * r + 2 * SUB, :].astype(F32)[:SUB]
        hi = pn_ref[2 * r + 2 * SUB:2 * r + 4 * SUB, :].astype(F32)[:SUB]
        pnt_ref[r:r + 2 * SUB, :] = jnp.concatenate([lo, hi], axis=0).astype(BF16)
    pl.semaphore_wait(barrier, 5)

    @pl.loop(0, HEAD)
    def _(t):
        x_copy(t).wait()
        x_copy(t + 1).start()

        @pl.when(t > 0)
        def _():
            p_copy(t - 1).start()

        @pl.when(t >= RING)
        def _():
            p_copy(t - RING).wait_send()

        lane = lax.broadcasted_iota(jnp.int32, (slots, tok), 1)
        base = s * tok
        stv = st[...]
        stl = lax.broadcasted_iota(jnp.int32, stv.shape, 1)
        x = xbuf[t % 2]
        lts = lax.dot_general(pnt_ref[...], row_unit(x), (((1,), (1,)), ((), ())), preferred_element_type=F32)
        es = []
        for i in range(nb):
            b = t * nb + i
            lt = lts[:, i * tok:(i + 1) * tok]
            valid = (base + lane) < len_ref[b]
            m = jnp.max(jnp.where(valid, lt, NEG_BIG), axis=1, keepdims=True)
            e = jnp.where(valid, jnp.exp(lt - m), 0.0)
            z = jnp.sum(e, axis=1, keepdims=True)
            stv = jnp.where(stl == b, m, jnp.where(stl == batch + b, z, stv))
            es.append(e.astype(BF16))
        nums = [jnp.dot(es[i], x[i * tok:(i + 1) * tok], preferred_element_type=F32) for i in range(nb)]
        for i in range(0, nb, 2):
            for u in range(NU):
                for q in range(NQ):
                    for rc in range(2):
                        r = ys_index(rc, u, q) * SUB
                        pair = jnp.concatenate([nums[i][r:r + SUB], nums[i + 1][r:r + SUB]], axis=0).astype(BF16)
                        if rc == 0:
                            keep[t, u, q, i * SUB:(i + 2) * SUB, :] = pair
                        else:
                            ring[t % RING, u, q, i * SUB:(i + 2) * SUB, :] = pair
        st[...] = stv

    p_copy(HEAD - 1).start()
    for k in range(3):
        st_copy(k).start()
    for n in range(WSLOT):
        for cp in e_copies(n):
            cp.start()
    for cp in w_copies():
        cp.wait()
    for k in range(3):
        st_copy(k).wait()

    @pl.loop(0, HEAD)
    def _(i):
        p_copy(i).wait_recv()

    for i in range(HEAD - RING, HEAD):
        p_copy(i).wait_send()

    def merge(u):
        @pl.loop(0, NQ)
        def _(n):
            q = NQ - 1 - n
            qx = (q + 2) % 4

            def stat(ref, rc, qq):
                return ref[pl.ds(pl.multiple_of(ys_index(rc, u, qq) * SUB, SUB), SUB), :]

            peers = (stat(st, 0, q), stat(st_in.at[0], 1, q), stat(st_in.at[1], 0, qx), stat(st_in.at[2], 1, qx))
            ms = [r[:, :batch] for r in peers]
            zs = [r[:, batch:] for r in peers]
            top = jnp.maximum(jnp.maximum(ms[0], ms[1]), jnp.maximum(ms[2], ms[3]))
            ws = [jnp.exp(m - top) for m in ms]
            inv = 1.0 / (ws[0] * zs[0] + ws[1] * zs[1] + ws[2] * zs[2] + ws[3] * zs[3])
            wk = ws[0] * inv
            wr = ws[1] * inv
            for i in range(HEAD):
                for j in range(0, nb, 2):
                    r = slice(j * SUB, (j + 2) * SUB)
                    kk = keep[i, u, q, r, :].astype(F32)
                    rr = recv[i, u, q, r, :].astype(F32)
                    both = []
                    for o in range(2):
                        b = i * nb + j + o
                        ro = slice(o * SUB, (o + 1) * SUB)
                        both.append(kk[ro] * wk[:, b:b + 1] + rr[ro] * wr[:, b:b + 1])
                    keep[i, u, q, r, :] = jnp.concatenate(both, axis=0).astype(BF16)

            @pl.when(n > 0)
            def _():
                d_copy(u, q + 1).start()

    merge(0)
    merge(1)

    def unpack(u):
        for q in (1, 2, 3):
            d_copy(u, q).wait_recv()

        @pl.loop(0, HEAD)
        def _(i):
            r = pl.ds(pl.multiple_of(i * rows, rows), rows)
            a = keep[i, u, 0].astype(F32) + drecv[u, 1, i].astype(F32)
            b = drecv[u, 0, i].astype(F32) + drecv[u, 2, i].astype(F32)
            for k in range(lanes):
                s_a[k, r, :] = a[:, k * 128:(k + 1) * 128]
                s_b[k, r, :] = b[:, k * 128:(k + 1) * 128]

    def pack(u):
        @pl.loop(0, HEAD)
        def _(i):
            r = pl.ds(pl.multiple_of(i * rows, rows), rows)
            for k in range(lanes):
                cols = slice(k * 128, (k + 1) * 128)
                recv[i, u, 0, :, cols] = s_a[k, r, :].astype(BF16)
                recv[i, u, 1, :, cols] = s_b[k, r, :].astype(BF16)

    def experts(u):
        unpack(u)

        @pl.loop(0, SUB)
        def _(e):
            pa = pl.ds(e, batch, stride=SUB)
            for k in range(lanes):
                cols = slice(k * 128, (k + 1) * 128)
                xs[:batch, cols] = s_a[k, pa, :].astype(BF16)
                xs[batch:, cols] = s_b[k, pa, :].astype(BF16)
            nc = 3
            fb = half_ff // nc
            xv = xs[...]

            def half(n):
                for cp in e_copies(n):
                    cp.wait()
                w = n % WSLOT

                def up(j):
                    return jnp.dot(xv, ew1[w, :, j * fb:(j + 1) * fb], preferred_element_type=F32)

                y = None
                h = up(0)
                for j in range(nc):
                    nxt = up(j + 1) if j + 1 < nc else None
                    v = jnp.dot(gelu(h).astype(BF16), ew2[w, j * fb:(j + 1) * fb, :], preferred_element_type=F32)
                    y = v if y is None else y + v
                    h = nxt

                @pl.when(n + WSLOT < 2 * owned)
                def _():
                    for cp in e_copies(n + WSLOT):
                        cp.start()

                return y

            n0 = 2 * (u * SUB + e)
            y = half(n0)
            for k in range(lanes):
                cols = slice(k * 128, (k + 1) * 128)
                s_a[k, pa, :] = y[:batch, cols]
                s_b[k, pa, :] = y[batch:, cols]
            y = half(n0 + 1)
            for k in range(lanes):
                cols = slice(k * 128, (k + 1) * 128)
                s_a[k, pa, :] += y[:batch, cols]
                s_b[k, pa, :] += y[batch:, cols]

        pack(u)

    def send_back(u):
        for q in (3, 2, 1):
            r_copy(u, q).start()
        own_copy(u).start()
        f_copy(u, 0).start()

    def forward(u, owners):
        for q in owners:
            r_copy(u, q).wait_recv()
            f_copy(u, q).start()

    def dense(j):
        n = HEAD + j
        k = j % 2
        x_copy(n).wait()

        @pl.when(j + 1 < HEAD)
        def _():
            x_copy(n + 1).start()

        @pl.when(j >= 2)
        def _():
            for cp in out_copies(j - 2):
                cp.wait()

        xn = row_unit(xbuf[n % 2])
        logits = lax.dot_general(xn, pn_ref[...], (((1,), (1,)), ((), ())), preferred_element_type=F32)
        ti = lax.broadcasted_iota(jnp.int32, logits.shape, 0)
        si = lax.broadcasted_iota(jnp.int32, logits.shape, 1)
        mine = ((ti // tok) % 2) == ((si // SUB) % 2)
        logits = jnp.where(mine, logits, NEG_BIG)
        ex = jnp.exp(logits - jnp.max(logits, axis=1, keepdims=True))
        cbuf[k] = (ex / jnp.sum(ex, axis=1, keepdims=True)).astype(BF16)
        nf = 3
        fb = ff // nf

        def up(f):
            return jnp.dot(xn, w1[:, f * fb:(f + 1) * fb], preferred_element_type=F32)

        h = up(0)
        for f in range(nf):
            nxt = up(f + 1) if f + 1 < nf else None
            y = jnp.dot(gelu(h).astype(BF16), w2[f * fb:(f + 1) * fb, :], preferred_element_type=F32)
            if f == 0:
                y2buf[k] = y
            else:
                y2buf[k] += y
            h = nxt
        for cp in out_copies(j):
            cp.start()

    for u in range(NU):
        @pl.loop(0, (D_A, D_B)[u])
        def _(j, u=u):
            dense(j + (0, D_A)[u])

        experts(u)
        send_back(u)

    @pl.loop(0, D_C)
    def _(j):
        for u in range(NU):

            @pl.when(j == T_FWD[u])
            def _(u=u):
                forward(u, (1, 3, 2) if u == 0 else (1, 3))

        dense(j + D_A + D_B)

    forward(1, (2,))
    for j in (HEAD - 2, HEAD - 1):
        for cp in out_copies(j):
            cp.wait()
    for u in range(NU):
        own_copy(u).wait()
        for q in (1, 2, 3):
            d_copy(u, q).wait_send()
            r_copy(u, q).wait_send()
        for q in range(NQ):
            f_copy(u, q).wait()


def step_call(lens, g, phi, x2, ws_in, ws_out, w_in, w_out, tok):
    tokens, width = x2.shape
    ff = ws_in.shape[1]
    slots = phi.shape[1]
    cols = 2 * slots
    tile = tokens // HEAD
    nb = tile // tok
    rows = nb * SUB
    batch = HEAD * nb
    hbm = pl.BlockSpec(memory_space=pl.ANY)
    dma = pltpu.SemaphoreType.DMA
    return pl.pallas_call(
        functools.partial(step_kernel, tok),
        in_specs=[
            pl.BlockSpec(memory_space=pltpu.SMEM),
            pl.BlockSpec(memory_space=pltpu.SMEM),
            pl.BlockSpec(memory_space=pltpu.VMEM),
            hbm, hbm, hbm, hbm, hbm,
        ],
        out_specs=[hbm, hbm, hbm],
        out_shape=[
            jax.ShapeDtypeStruct((tokens, width), F32),
            jax.ShapeDtypeStruct((tokens, cols), BF16),
            jax.ShapeDtypeStruct((2 * NU * NQ, HEAD, rows, width), BF16),
        ],
        scratch_shapes=[
            pltpu.VMEM((slots, width), F32),
            pltpu.VMEM((slots, width), BF16),
            pltpu.VMEM((cols, width), BF16),
            pltpu.VMEM((2, tile, width), BF16),
            pltpu.VMEM((2, tile, width), F32),
            pltpu.VMEM((2, tile, cols), BF16),
            pltpu.VMEM((RING, NU, NQ, rows, width), BF16),
            pltpu.VMEM((HEAD, NU, NQ, rows, width), BF16),
            pltpu.VMEM((HEAD, NU, NQ, rows, width), BF16),
            pltpu.VMEM((NU, 3, HEAD, rows, width), BF16),
            pltpu.VMEM((slots, 2 * batch), F32),
            pltpu.VMEM((3, slots, 2 * batch), F32),
            pltpu.VMEM((width, ff), BF16),
            pltpu.VMEM((ff, width), BF16),
            pltpu.VMEM((WSLOT, width, ff // 2), BF16),
            pltpu.VMEM((WSLOT, ff // 2, width), BF16),
            pltpu.VMEM((width // 128, batch * SUB, 128), F32),
            pltpu.VMEM((width // 128, batch * SUB, 128), F32),
            pltpu.VMEM((2 * batch, width), BF16),
            dma((2,)), dma((2,)), dma((2,)),
            dma((RING,)), dma((HEAD,)), dma((3,)), dma((3,)),
            dma((NU, 3)), dma((NU, 3)), dma((NU, 3)), dma((NU, 3)), dma((NU,)),
            dma((NU, NQ)), dma((NU, NQ)), dma((2,)), dma((2, WSLOT)),
        ],
        compiler_params=pltpu.CompilerParams(vmem_limit_bytes=67043328, collective_id=0, has_side_effects=True),
        cost_estimate=pl.CostEstimate(flops=6 * tokens * width * ff, bytes_accessed=4 * SUB * NU * width * ff, transcendentals=tokens * ff),
        name="steps",
    )(lens, g, phi, x2, ws_in, ws_out, w_in, w_out)


def combine_kernel(tok, c_ref, y2_ref, ys_ref, out_ref):
    n_arr, blocks, rows, _ = ys_ref.shape
    pairs = rows // (2 * SUB)
    for p in range(blocks * pairs):
        lo = (p % pairs) * 2 * SUB
        ys = jnp.concatenate([ys_ref[a, p // pairs, lo:lo + 2 * SUB, :] for a in range(n_arr)], axis=0)
        r = slice(p * 2 * tok, (p + 1) * 2 * tok)
        y1 = jnp.dot(c_ref[r, :], ys, preferred_element_type=F32)
        out_ref[r, :] = (y1 + y2_ref[r, :]).astype(BF16)


def combine_call(c, y2, ys, tok):
    tokens, width = y2.shape
    n_arr, steps, rows, _ = ys.shape
    blocks = 2
    steps //= blocks
    tile = tokens // steps
    return pl.pallas_call(
        functools.partial(combine_kernel, tok),
        grid=(steps,),
        in_specs=[
            pl.BlockSpec((tile, c.shape[1]), lambda i: (i, 0)),
            pl.BlockSpec((tile, width), lambda i: (i, 0)),
            pl.BlockSpec((n_arr, blocks, rows, width), lambda i: (0, i, 0, 0)),
        ],
        out_specs=pl.BlockSpec((tile, width), lambda i: (i, 0)),
        out_shape=jax.ShapeDtypeStruct((tokens, width), BF16),
        compiler_params=params(("arbitrary",), 60),
        cost_estimate=pl.CostEstimate(flops=2 * tokens * width * c.shape[1], bytes_accessed=8 * tokens * width, transcendentals=0),
        name="combine",
    )(c, y2, ys)


def solution(mesh):
    tok_spec = P('data', 'seq', None)
    expert_spec = P('seq', None, None)

    def per_device(x_blk, len_blk, phi_slots, scale_g, w_in, w_out, ws_in, ws_out):
        batch, tok, width = x_blk.shape
        x2 = x_blk.reshape(batch * tok, width)
        y2, c, ys = step_call(len_blk, scale_g.reshape(1), phi_slots, x2, ws_in, ws_out, w_in, w_out, tok)
        return combine_call(c, y2, ys, tok).reshape(batch, tok, width)

    return jax.shard_map(per_device, mesh=mesh, in_specs=(tok_spec, P('data'), P(), P(), expert_spec, expert_spec, P(), P()), out_specs=tok_spec, check_vma=False)
```
